32 devices in a mesh: batch: 1 (over z), time: 4 (over y), region: 8 (over x, core).
Axes of the slice: x: 4, y: 4, z: 1, core: 2. Of those that a mesh axis runs over, the one named last changes fastest.
The devices are a block of a 4x4x8 slice.
Arguments:
- patches: bfloat16 [2048, 768], P(('batch', 'time', 'region'))
- enc_pos: bfloat16 [2048, 1024], P(('batch', 'time', 'region'))
- vis_mask: int32 [2048], P(('batch', 'time', 'region'))
- dec_pos: bfloat16 [2048, 512], P(('batch', 'time', 'region'))
- w_embed: bfloat16 [768, 1024], replicated
- b_embed: float32 [1024], replicated
- enc_vec: float32 [2, 12, 1024], replicated
- enc_wqkv: bfloat16 [2, 1024, 3, 16, 64], replicated
- enc_wo: bfloat16 [2, 16, 64, 1024], replicated
- enc_w1: bfloat16 [2, 1024, 4096], replicated
- enc_w2: bfloat16 [2, 4096, 1024], replicated
- enc_final: float32 [2, 1024], replicated
- w_dec_in: bfloat16 [1024, 512], replicated
- mask_token: bfloat16 [512], replicated
- dec_vec: float32 [2, 12, 512], replicated
- dec_wqkv: bfloat16 [2, 512, 3, 16, 32], replicated
- dec_wo: bfloat16 [2, 16, 32, 512], replicated
- dec_w1: bfloat16 [2, 512, 2048], replicated
- dec_w2: bfloat16 [2, 2048, 512], replicated
- dec_final: float32 [2, 512], replicated
- w_out: bfloat16 [512, 768], replicated
Outputs:
- output: float32 [2048, 768], P(('batch', 'time', 'region'))
All inputs are finite; a program needn't handle non-finite values.
Results may differ from the reference program's by a relative error of at most 0.016158.
Values are sent between devices in bfloat16 or wider.
A program may use at most 768 MiB of HBM per device.

```python
import jax
import jax.numpy as jnp
from jax import lax

PATCH_DIM = 768
ENC_WIDTH = 1024
ENC_HEADS = 16
DEC_WIDTH = 512
DEC_HEADS = 16
TOKENS_DEV = 64
TIME_BLOCKS = 4
REGIONS = 8
KEEP_DIV = 8
ENC_LAYERS = 2
DEC_LAYERS = 2

SHARDS = TIME_BLOCKS * REGIONS
TOKENS = TOKENS_DEV * SHARDS
VIS_DEV = TOKENS_DEV // KEEP_DIV
VISIBLE = VIS_DEV * SHARDS
SKEW = min(4, REGIONS)
ENC_HEAD = ENC_WIDTH // ENC_HEADS
DEC_HEAD = DEC_WIDTH // DEC_HEADS
LN_EPS = 1e-6


def draw_mask(mask_key):
    key_rank, key_shift, key_place = jax.random.split(mask_key, 3)
    pair_count = (REGIONS - SKEW) // 2
    shifts = jax.random.randint(key_shift, (TIME_BLOCKS, pair_count), 0, VIS_DEV + 1)
    paired = jnp.stack([VIS_DEV + shifts, VIS_DEV - shifts], axis=-1).reshape(TIME_BLOCKS, REGIONS - SKEW)
    profile = jnp.concatenate([jnp.full((TIME_BLOCKS, 1), SKEW * VIS_DEV, jnp.int32), jnp.zeros((TIME_BLOCKS, SKEW - 1), jnp.int32), paired.astype(jnp.int32)], axis=1)
    region_rank = jax.vmap(lambda one_key: jax.random.permutation(one_key, REGIONS))(jax.random.split(key_rank, TIME_BLOCKS))
    counts = jnp.take_along_axis(profile, region_rank, axis=1).reshape(SHARDS, 1)
    token_rank = jax.vmap(lambda one_key: jax.random.permutation(one_key, TOKENS_DEV))(jax.random.split(key_place, SHARDS))
    return (token_rank < counts).astype(jnp.int32).reshape(TOKENS)


def normal_draw(draw_key, out_shape, spread):
    return jax.random.normal(draw_key, out_shape, jnp.float32) * spread


def qkv_gain():
    return jnp.array([1.6, 1.6, 1.0], jnp.float32)[:, None, None]


def block_vectors(draw_key, layer_count, model_width):
    gain_rows = jnp.array([1.0, 0.0, 1.0, 0.0, 0.0, 0.0, 0.0, 0.0, 0.0, 0.0, 0.0, 0.0], jnp.float32)[:, None]
    return jax.random.normal(draw_key, (layer_count, 12, model_width), jnp.float32) * 0.2 + gain_rows


def final_vectors(draw_key, model_width):
    return jax.random.normal(draw_key, (2, model_width), jnp.float32) * 0.2 + jnp.array([1.0, 0.0], jnp.float32)[:, None]


def setup_inputs(seed: int = 0, part: int = 0) -> dict:
    part_key = jax.random.fold_in(jax.random.key(seed), part)
    key_patch, key_epos, key_mask, key_dpos = jax.random.split(part_key, 4)
    weight_keys = jax.random.split(jax.random.key(seed + 1), 17)
    return {
        "patches": normal_draw(key_patch, (TOKENS, PATCH_DIM), 1.0).astype(jnp.bfloat16),
        "enc_pos": normal_draw(key_epos, (TOKENS, ENC_WIDTH), 0.5).astype(jnp.bfloat16),
        "vis_mask": draw_mask(key_mask),
        "dec_pos": normal_draw(key_dpos, (TOKENS, DEC_WIDTH), 0.5).astype(jnp.bfloat16),
        "w_embed": normal_draw(weight_keys[0], (PATCH_DIM, ENC_WIDTH), PATCH_DIM ** -0.5).astype(jnp.bfloat16),
        "b_embed": normal_draw(weight_keys[1], (ENC_WIDTH,), 0.5),
        "enc_vec": block_vectors(weight_keys[2], ENC_LAYERS, ENC_WIDTH),
        "enc_wqkv": (normal_draw(weight_keys[3], (ENC_LAYERS, ENC_WIDTH, 3, ENC_HEADS, ENC_HEAD), ENC_WIDTH ** -0.5) * qkv_gain()).astype(jnp.bfloat16),
        "enc_wo": normal_draw(weight_keys[4], (ENC_LAYERS, ENC_HEADS, ENC_HEAD, ENC_WIDTH), 1.5 * ENC_WIDTH ** -0.5).astype(jnp.bfloat16),
        "enc_w1": normal_draw(weight_keys[5], (ENC_LAYERS, ENC_WIDTH, 4 * ENC_WIDTH), ENC_WIDTH ** -0.5).astype(jnp.bfloat16),
        "enc_w2": normal_draw(weight_keys[6], (ENC_LAYERS, 4 * ENC_WIDTH, ENC_WIDTH), (4 * ENC_WIDTH) ** -0.5).astype(jnp.bfloat16),
        "enc_final": final_vectors(weight_keys[7], ENC_WIDTH),
        "w_dec_in": normal_draw(weight_keys[8], (ENC_WIDTH, DEC_WIDTH), 1.5 * ENC_WIDTH ** -0.5).astype(jnp.bfloat16),
        "mask_token": normal_draw(weight_keys[9], (DEC_WIDTH,), 1.0).astype(jnp.bfloat16),
        "dec_vec": block_vectors(weight_keys[10], DEC_LAYERS, DEC_WIDTH),
        "dec_wqkv": (normal_draw(weight_keys[11], (DEC_LAYERS, DEC_WIDTH, 3, DEC_HEADS, DEC_HEAD), DEC_WIDTH ** -0.5) * qkv_gain()).astype(jnp.bfloat16),
        "dec_wo": normal_draw(weight_keys[12], (DEC_LAYERS, DEC_HEADS, DEC_HEAD, DEC_WIDTH), 1.5 * DEC_WIDTH ** -0.5).astype(jnp.bfloat16),
        "dec_w1": normal_draw(weight_keys[13], (DEC_LAYERS, DEC_WIDTH, 4 * DEC_WIDTH), DEC_WIDTH ** -0.5).astype(jnp.bfloat16),
        "dec_w2": normal_draw(weight_keys[14], (DEC_LAYERS, 4 * DEC_WIDTH, DEC_WIDTH), (4 * DEC_WIDTH) ** -0.5).astype(jnp.bfloat16),
        "dec_final": final_vectors(weight_keys[15], DEC_WIDTH),
        "w_out": normal_draw(weight_keys[16], (DEC_WIDTH, PATCH_DIM), DEC_WIDTH ** -0.5).astype(jnp.bfloat16),
    }


def layer_norm(hidden, ln_gain, ln_shift):
    hid_f32 = hidden.astype(jnp.float32)
    mean_val = jnp.mean(hid_f32, axis=-1, keepdims=True)
    centered = hid_f32 - mean_val
    variance = jnp.mean(centered * centered, axis=-1, keepdims=True)
    return centered * lax.rsqrt(variance + LN_EPS) * ln_gain + ln_shift


def attention(query_rows, key_rows, value_rows, blocks):
    query_count, head_count, head_dim = query_rows.shape
    q_blocks = query_rows.reshape(blocks, query_count // blocks, head_count, head_dim)
    key_f32 = key_rows.astype(jnp.float32)
    value_f32 = value_rows.astype(jnp.float32)

    def one_block(q_block):
        scores = jnp.einsum("qhd,khd->hqk", q_block.astype(jnp.float32), key_f32) * (head_dim ** -0.5)
        attn_probs = jax.nn.softmax(scores, axis=-1).astype(jnp.bfloat16)
        return jnp.einsum("hqk,khd->qhd", attn_probs.astype(jnp.float32), value_f32).astype(jnp.bfloat16)

    return lax.map(one_block, q_blocks).reshape(query_count, head_count, head_dim)


def transformer_block(hidden, vec_rows, w_qkv, w_o, w_one, w_two, blocks):
    head_count, head_dim = w_qkv.shape[2], w_qkv.shape[3]
    normed = layer_norm(hidden, vec_rows[0], vec_rows[1]).astype(jnp.bfloat16)
    qkv_bias = jnp.stack([vec_rows[4], jnp.zeros_like(vec_rows[4]), vec_rows[5]]).reshape(1, 3, head_count, head_dim)
    qkv_rows = (jnp.einsum("nd,dche->nche", normed.astype(jnp.float32), w_qkv.astype(jnp.float32)) + qkv_bias).astype(jnp.bfloat16)
    attended = attention(qkv_rows[:, 0], qkv_rows[:, 1], qkv_rows[:, 2], blocks)
    residual = (hidden.astype(jnp.float32) + jnp.einsum("nhe,hed->nd", attended.astype(jnp.float32), w_o.astype(jnp.float32)) + vec_rows[6]).astype(jnp.bfloat16)
    normed_mlp = layer_norm(residual, vec_rows[2], vec_rows[3]).astype(jnp.bfloat16)
    mlp_hidden = jax.nn.gelu(jnp.dot(normed_mlp, w_one, preferred_element_type=jnp.float32) + vec_rows[8:12].reshape(-1), approximate=False).astype(jnp.bfloat16)
    return (residual.astype(jnp.float32) + jnp.dot(mlp_hidden, w_two, preferred_element_type=jnp.float32) + vec_rows[7]).astype(jnp.bfloat16)


def run_stack(hidden, vec_stack, wqkv_stack, wo_stack, w1_stack, w2_stack, blocks):
    def layer_step(hidden_state, layer_params):
        vec_rows, w_qkv, w_o, w_one, w_two = layer_params
        return transformer_block(hidden_state, vec_rows, w_qkv, w_o, w_one, w_two, blocks), None

    final_state, _ = lax.scan(layer_step, hidden, (vec_stack, wqkv_stack, wo_stack, w1_stack, w2_stack))
    return final_state


def reference(patches, enc_pos, vis_mask, dec_pos, w_embed, b_embed, enc_vec, enc_wqkv, enc_wo, enc_w1, enc_w2, enc_final, w_dec_in, mask_token, dec_vec, dec_wqkv, dec_wo, dec_w1, dec_w2, dec_final, w_out):
    vis_idx = jnp.nonzero(vis_mask, size=VISIBLE)[0]
    embedded = (jnp.dot(patches[vis_idx], w_embed, preferred_element_type=jnp.float32) + b_embed + enc_pos[vis_idx].astype(jnp.float32)).astype(jnp.bfloat16)
    encoded = run_stack(embedded, enc_vec, enc_wqkv, enc_wo, enc_w1, enc_w2, SHARDS)
    latent = jnp.dot(layer_norm(encoded, enc_final[0], enc_final[1]).astype(jnp.bfloat16), w_dec_in, preferred_element_type=jnp.float32).astype(jnp.bfloat16)
    scattered = jnp.zeros((TOKENS, DEC_WIDTH), jnp.float32).at[vis_idx].set(latent.astype(jnp.float32))
    dec_in = (jnp.where(vis_mask[:, None] == 1, scattered, mask_token.astype(jnp.float32)) + dec_pos.astype(jnp.float32)).astype(jnp.bfloat16)
    decoded = run_stack(dec_in, dec_vec, dec_wqkv, dec_wo, dec_w1, dec_w2, SHARDS)
    return jnp.dot(layer_norm(decoded, dec_final[0], dec_final[1]).astype(jnp.bfloat16), w_out, preferred_element_type=jnp.float32)
```

```python
import functools
import jax
import jax.numpy as jnp
from jax import lax
from jax.experimental import pallas as pl
from jax.experimental.pallas import tpu as pltpu
from jax.sharding import PartitionSpec as P

KEEP_DIV = 8
LN_EPS = 1e-6
CORES = 2
TOKEN_AXES = ("batch", "time", "region")
MESH_ID = pl.DeviceIdType.MESH
F32 = jnp.float32
BF16 = jnp.bfloat16
LOG2E = 1.4426950408889634


def mm(lhs, rhs):
    return jnp.dot(lhs, rhs, preferred_element_type=F32)


def mm_t(lhs, rhs):
    return lax.dot_general(lhs, rhs, (((1,), (1,)), ((), ())), preferred_element_type=F32)


def norm(rows, gain, shift):
    rows = rows.astype(F32)
    centered = rows - jnp.mean(rows, axis=-1, keepdims=True)
    variance = jnp.mean(centered * centered, axis=-1, keepdims=True)
    return (centered * lax.rsqrt(variance + LN_EPS) * gain + shift).astype(BF16)


def gelu(val):
    return 0.5 * val * (1.0 + lax.erf(val * 0.7071067811865476))


def loop(count, body):
    lax.fori_loop(0, count, lambda i, c: (body(i), c)[1], 0)


def blk(i, size):
    return pl.ds(pl.multiple_of(i * size, size), size)


def column_of(row, lanes):
    return jnp.broadcast_to(row, (lanes, row.shape[1])).T


def head_rows(q_rows, heads):
    lanes = q_rows.shape[1]
    head = lax.broadcasted_iota(jnp.int32, q_rows.shape, 1) // (lanes // heads)
    return jnp.concatenate([jnp.where(head == h, q_rows, jnp.zeros_like(q_rows)) for h in range(heads)], axis=0)


def unstack_heads(out_t, heads):
    out = out_t.T
    rows = out.shape[0] // heads
    head = lax.broadcasted_iota(jnp.int32, (rows, out.shape[1]), 1) // (out.shape[1] // heads)
    total = jnp.where(head == 0, out[:rows], 0.0)
    for h in range(1, heads):
        total = total + jnp.where(head == h, out[h * rows:(h + 1) * rows], 0.0)
    return total


def kernel(nt, nr, patches, enc_pos, vis, dec_pos, b_embed, evec, efin, mtok, dvec, dfin,
           w_embed, wqkv, wo, w1, w2, w_dec, dqkv, dwo, dw1, dw2, w_out,
           out,
           X0, X1, Y0, Y1, Z0, SL, MT, MB, E, H1, H2, A, Q, K, VT, ATT, HM, Z, ZT, DP, A2, S, PR, HD,
           wsem, s_e, r_e, s_g, r_g, s_h, r_h):
    t = lax.axis_index("time")
    r = lax.axis_index("region")
    nx = nr // CORES
    x, core = r // CORES, lax.rem(r, CORES)
    partner = r + 1 - 2 * core
    tok = patches.shape[0]
    slots = SL.shape[1]
    vis_blk = E.shape[0] // nt
    ed, dd = E.shape[1], dec_pos.shape[1]
    nvis = E.shape[0]

    def xpeer(dx):
        return lax.rem(x + dx, nx) * CORES + core

    def tpeer(dy):
        return lax.rem(t + dy, nt)

    def xsrc(dx):
        return lax.rem(x + nx - dx, nx) * CORES + core

    def tsrc(dy):
        return lax.rem(t + nt - dy, nt)

    def rcopy(src, dst, ssem, rsem, tt, rr):
        return pltpu.make_async_remote_copy(src_ref=src, dst_ref=dst, send_sem=ssem, recv_sem=rsem,
                                            device_id={"time": tt, "region": rr}, device_id_type=MESH_ID)

    def load(src, dst, i):
        return pltpu.make_async_copy(src, dst, wsem.at[i])

    ld_embed = load(w_embed, Y1.at[0:w_embed.shape[0], 0:ed], 0)
    ld_embed.start()

    barrier = pltpu.get_barrier_semaphore()
    peers = [(t, partner)] + [(t, xpeer(d)) for d in range(1, nx)] + [(tpeer(d), r) for d in range(1, nt)]
    for tt, rr in peers:
        pl.semaphore_signal(barrier, inc=1, device_id={"time": tt, "region": rr}, device_id_type=MESH_ID)

    mask_row = vis[...].astype(F32)
    mask_pad = jnp.concatenate([mask_row, jnp.zeros((1, 128 - tok), F32)], axis=1)
    MT[r] = jnp.broadcast_to(mask_pad, (8, 128))
    tri = (lax.broadcasted_iota(jnp.int32, (128, 128), 0) < lax.broadcasted_iota(jnp.int32, (128, 128), 1)).astype(BF16)
    local_rank = mm(jnp.broadcast_to(mask_pad, (8, 128)).astype(BF16), tri)[0:1, 0:tok]
    slot_id = lax.broadcasted_iota(jnp.int32, (slots, tok), 0).astype(F32)
    selector = jnp.where((local_rank == slot_id) & (mask_row == 1.0), 1.0, 0.0).astype(BF16)

    ld_embed.wait()
    qkv_w, d_w = 3 * ed, 3 * dd
    ld_a = [load(wqkv.at[0], X0.at[0:qkv_w], 1), load(wo.at[0], X0.at[qkv_w:qkv_w + ed], 2)]
    ld_b = [load(w1.at[0], Y0, 3), load(w2.at[0], Z0, 4)]
    ld_c = [load(wqkv.at[1], X1.at[0:qkv_w], 5), load(wo.at[1], X1.at[qkv_w:qkv_w + ed], 6)]
    for cp in ld_a + ld_b + ld_c:
        cp.start()

    def embed_cols(j):
        cols = blk(j, 256)
        emb = (mm(patches[...], Y1[0:patches.shape[1], cols]) + b_embed[:, cols] + enc_pos[:, cols].astype(F32)).astype(BF16)
        SL[r, :, cols] = mm(selector, emb).astype(BF16)

    loop(ed // 256, embed_cols)
    ld_d = load(w1.at[1], Y1, 7)
    ld_d.start()
    pl.semaphore_wait(barrier, len(peers))

    st = []
    for i, rr in enumerate([partner] + [xpeer(d) for d in range(1, nx)]):
        st.append(rcopy(SL.at[r], SL.at[r], s_e.at[i], r_e.at[i], t, rr))
        st.append(rcopy(MT.at[r], MT.at[r], s_e.at[8 + i], r_e.at[8 + i], t, rr))
    for cp in st:
        cp.start()
    fw = []
    for d in range(1, nx):
        src = xsrc(d)
        rcopy(SL.at[src], SL.at[src], s_e.at[d], r_e.at[d], t, r).wait_recv()
        rcopy(MT.at[src], MT.at[src], s_e.at[8 + d], r_e.at[8 + d], t, r).wait_recv()
        one = rcopy(SL.at[src], SL.at[src], s_e.at[16 + d], r_e.at[16 + d], t, partner)
        two = rcopy(MT.at[src], MT.at[src], s_e.at[24 + d], r_e.at[24 + d], t, partner)
        one.start()
        two.start()
        fw += [one, two]
    rcopy(SL.at[partner], SL.at[partner], s_e.at[0], r_e.at[0], t, r).wait_recv()
    rcopy(MT.at[partner], MT.at[partner], s_e.at[8], r_e.at[8], t, r).wait_recv()
    for cp in fw:
        cp.wait_recv()

    mask_all = jnp.concatenate([MT[d, 0:1, :] for d in range(nr)], axis=0)
    MB[t] = mask_all
    counts = jnp.sum(mask_all, axis=1, keepdims=True)
    lane_dev = lax.broadcasted_iota(jnp.int32, (nr, nr * slots), 1) // slots
    sub_dev = lax.broadcasted_iota(jnp.int32, (nr, nr * slots), 0)
    lane_cnt = jnp.sum(jnp.where(lane_dev == sub_dev, counts, 0.0), axis=0, keepdims=True)
    lane_off = jnp.sum(jnp.where(sub_dev < lane_dev, counts, 0.0), axis=0, keepdims=True)
    lane_slot = lax.rem(lax.broadcasted_iota(jnp.int32, (1, nr * slots), 1), slots).astype(F32)
    target = jnp.where(lane_slot < lane_cnt, lane_off + lane_slot, -1.0)
    rank_id = lax.broadcasted_iota(jnp.int32, (vis_blk, nr * slots), 0).astype(F32)
    compact = jnp.where(target == rank_id, 1.0, 0.0).astype(BF16)
    my_rows = blk(t, vis_blk)

    def compact_cols(j):
        cols = blk(j, 256)
        E[my_rows, cols] = mm(compact, SL[:, :, cols].reshape(nr * slots, 256)).astype(BF16)

    loop(ed // 256, compact_cols)

    half = vis_blk // CORES
    st2 = []
    for d in range(1, nt):
        rows = pl.ds(pl.multiple_of(t * vis_blk + core * half, half), half)
        st2.append(rcopy(E.at[rows], E.at[rows], s_e.at[32 + d], r_e.at[32 + d], tpeer(d), r))
        st2.append(rcopy(MB.at[t], MB.at[t], s_e.at[40 + d], r_e.at[40 + d], tpeer(d), r))
    for cp in st2:
        cp.start()
    DP[t, r] = dec_pos[...]

    def gather(buf, ss, rs):
        hw = dd // 2
        first, second, third = [], [], []

        def step1():
            first.append(rcopy(buf.at[t, r], buf.at[t, r], ss.at[0], rs.at[0], t, partner))
            for d in range(1, nt):
                first.append(rcopy(buf.at[t, r], buf.at[t, r], ss.at[d], rs.at[d], tpeer(d), r))
            for d in range(1, nx):
                first.append(rcopy(buf.at[t, r], buf.at[t, r], ss.at[4 + d], rs.at[4 + d], t, xpeer(d)))
            for cp in first:
                cp.start()

        def to_partner(ref, i):
            cp = rcopy(ref, ref, ss.at[i], rs.at[i], t, partner)
            cp.start()
            third.append(cp)

        def step2():
            for d in range(1, max(nt, nx)):
                if d < nt:
                    src = tsrc(d)
                    rcopy(buf.at[src, r], buf.at[src, r], ss.at[d], rs.at[d], t, r).wait_recv()
                    for e in range(1, nx):
                        i = 8 + d * 4 + e
                        half_ref = buf.at[src, r, :, 0:hw]
                        cp = rcopy(half_ref, half_ref, ss.at[i], rs.at[i], t, xpeer(e))
                        cp.start()
                        second.append(cp)
                    to_partner(buf.at[src, r], 40 + d * 4)
                if d < nx:
                    src = xsrc(d)
                    rcopy(buf.at[t, src], buf.at[t, src], ss.at[4 + d], rs.at[4 + d], t, r).wait_recv()
                    for e in range(1, nt):
                        i = 24 + d * 4 + e
                        half_ref = buf.at[t, src, :, hw:dd]
                        cp = rcopy(half_ref, half_ref, ss.at[i], rs.at[i], tpeer(e), r)
                        cp.start()
                        second.append(cp)
                    to_partner(buf.at[t, src], 40 + d)

        def step3():
            for d in range(1, nt):
                for e in range(1, nx):
                    low = buf.at[tsrc(d), xsrc(e), :, 0:hw]
                    high = buf.at[tsrc(d), xsrc(e), :, hw:dd]
                    rcopy(low, low, ss.at[8 + d * 4 + e], rs.at[8 + d * 4 + e], t, r).wait_recv()
                    rcopy(high, high, ss.at[24 + e * 4 + d], rs.at[24 + e * 4 + d], t, r).wait_recv()
                    to_partner(buf.at[tsrc(d), xsrc(e)], 40 + d * 4 + e)

        def finish():
            rcopy(buf.at[t, partner], buf.at[t, partner], ss.at[0], rs.at[0], t, r).wait_recv()
            for cp in third:
                cp.wait_recv()

        def drain():
            for cp in first + second + third:
                cp.wait_send()

        return step1, step2, step3, finish, drain

    g1 = gather(DP, s_g, r_g)
    g1[0]()

    fw2 = []
    for d in range(1, nt):
        rows = pl.ds(pl.multiple_of(tsrc(d) * vis_blk + core * half, half), half)
        rcopy(E.at[rows], E.at[rows], s_e.at[32 + d], r_e.at[32 + d], t, r).wait_recv()
        cp = rcopy(E.at[rows], E.at[rows], s_e.at[48 + d], r_e.at[48 + d], t, partner)
        cp.start()
        fw2.append(cp)
        rcopy(MB.at[tsrc(d)], MB.at[tsrc(d)], s_e.at[40 + d], r_e.at[40 + d], t, r).wait_recv()
    for d in range(1, nt):
        rows = pl.ds(pl.multiple_of(tsrc(d) * vis_blk + (1 - core) * half, half), half)
        rcopy(E.at[rows], E.at[rows], s_e.at[48 + d], r_e.at[48 + d], t, r).wait_recv()

    def norm_rows(src, dst, count, gain, shift, start=0, step=32):
        def body(i):
            rows = pl.ds(pl.multiple_of(start + i * step, step), step)
            dst[blk(i, step), :] = norm(src[rows, :], gain, shift)
        loop(count // step, body)

    def project(dst, rows_n, src_rows, w, w_row, bias):
        def body(j):
            cols = blk(j, 512)
            acc = mm_t(A[src_rows, :], w[pl.ds(pl.multiple_of(w_row + j * 512, 512), 512), :])
            if bias is not None:
                acc = acc + bias(cols)
            dst[0:rows_n, cols] = acc.astype(BF16)
        loop(ed // 512, body)

    def enc_layer(layer, w_a, w_up, w_down, src, rows_n, start, wait_down):
        def vec(i):
            return evec[i, layer:layer + 1, :]

        norm_rows(src, A, nvis, vec(0), vec(1))
        q_rows = pl.ds(pl.multiple_of(start, rows_n), rows_n)
        project(Q, rows_n, q_rows, w_a, 0, lambda cols: evec[4, layer:layer + 1, cols])
        project(K, nvis, slice(None), w_a, ed, None)

        def v_rows(j):
            rows = blk(j, 256)
            bias = column_of(evec[5, layer:layer + 1, rows], 128)
            acc = mm_t(w_a[pl.ds(pl.multiple_of(2 * ed + j * 256, 256), 256), :], A[...])
            VT[rows, :] = (acc + jnp.concatenate([bias] * (nvis // 128), axis=1)).astype(BF16)

        loop(ed // 256, v_rows)

        def heads2(p):
            cols = blk(p, 128)
            scores = mm_t(K[:, cols], head_rows(Q[0:rows_n, cols], 2))
            top = jnp.max(scores, axis=0, keepdims=True)
            ex = jnp.exp2((scores - top) * (0.125 * LOG2E))
            prob = (ex * (1.0 / jnp.sum(ex, axis=0, keepdims=True))).astype(BF16)
            ATT[0:rows_n, cols] = unstack_heads(mm(VT[cols, :], prob), 2).astype(BF16)

        loop(ed // 128, heads2)

        def out_cols(j):
            cols = blk(j, 512)
            acc = src[q_rows, cols].astype(F32) + mm(ATT[0:rows_n, :], w_a[3 * ed:4 * ed, cols])
            H1[0:rows_n, cols] = (acc + evec[6, layer:layer + 1, cols]).astype(BF16)

        loop(ed // 512, out_cols)
        wait_down()
        norm_rows(H1, A, rows_n, vec(2), vec(3))

        def up_cols(j):
            half_cols = blk(lax.rem(j, ed // 512), 512)
            acc = mm(A[0:rows_n, :], w_up[:, blk(j, 512)])
            HM[0:rows_n, blk(j, 512)] = gelu(acc + evec[8 + j // (ed // 512), layer:layer + 1, half_cols]).astype(BF16)

        loop(w_up.shape[1] // 512, up_cols)

        def down_cols(j):
            cols = blk(j, 256)
            acc = H1[0:rows_n, cols].astype(F32) + mm(HM[0:rows_n, :], w_down[:, cols])
            H2[0:rows_n, cols] = (acc + evec[7, layer:layer + 1, cols]).astype(BF16)

        loop(ed // 256, down_cols)

    for cp in ld_a:
        cp.wait()
    ld_e = load(w2.at[1], X0, 8)

    def mid0():
        ld_e.start()
        g1[1]()
        for cp in ld_b:
            cp.wait()

    enc_layer(0, X0, Y0, Z0, E, nvis, 0, mid0)
    dh = w_dec.shape[0]
    ld_f = []
    for l in range(2):
        ld_f.append(load(dqkv.at[l], Z0.at[l * d_w:(l + 1) * d_w, 0:dd], 9 + l))
        ld_f.append(load(dwo.at[l], Z0.at[2 * d_w + l * dd:2 * d_w + (l + 1) * dd, 0:dd], 11 + l))
        ld_f.append(load(dw1.at[l], Y0.at[l * dd:(l + 1) * dd, 0:4 * dd], 13 + l))
        ld_f.append(load(dw2.at[l], Z0.at[l * 4 * dd:(l + 1) * 4 * dd, dd:2 * dd], 15 + l))
    ld_f.append(load(w_out, Y0.at[0:dd, 4 * dd:4 * dd + w_out.shape[1]], 17))
    ld_dec = load(w_dec, Y0.at[0:dh, 6 * dd:7 * dd], 18)
    ld_dec.start()
    for cp in ld_f:
        cp.start()
    for cp in ld_c:
        cp.wait()

    def mid1():
        g1[2]()
        ld_d.wait()
        ld_e.wait()

    enc_layer(1, X1, Y1, X0, H2, vis_blk, t * vis_blk, mid1)
    norm_rows(H2, A, vis_blk, efin[0:1, :], efin[1:2, :])
    ld_dec.wait()
    Z[t] = mm(A[0:vis_blk, :], Y0[0:dh, 6 * dd:7 * dd]).astype(BF16)
    stz = []
    for d in range(1, nt):
        stz.append(rcopy(Z.at[t], Z.at[t], s_e.at[56 + d], r_e.at[56 + d], tpeer(d), r))
    for cp in stz:
        cp.start()
    g1[3]()
    for cp in ld_f:
        cp.wait()

    heads_g = 4
    ntok = nt * nr * tok

    def keys_values(layer, a_rows, c):
        rows = blk(c, 256)
        base = layer * d_w
        X1[rows, 0:dd] = mm_t(a_rows, Z0[base + dd:base + 2 * dd, 0:dd]).astype(BF16)
        acc = mm_t(Z0[base + 2 * dd:base + 3 * dd, 0:dd], a_rows)
        bias = column_of(dvec[5, layer:layer + 1, :], 128)
        Y1[0:dd, rows] = (acc + jnp.concatenate([bias] * 2, axis=1)).astype(BF16)

    for d in range(1, nt):
        src = tsrc(d)
        rcopy(Z.at[src], Z.at[src], s_e.at[56 + d], r_e.at[56 + d], t, r).wait_recv()

    per = 256 // tok
    tri_b = tri

    def first_chunk(c):
        tb = c // (nr // per)
        dev0 = lax.rem(c, nr // per) * per
        masks = MB[tb]
        ranks = mm(masks.astype(BF16), tri_b)
        cnt = jnp.sum(masks, axis=1, keepdims=True)
        sub = lax.broadcasted_iota(jnp.int32, (nr, nr), 0)
        lane = lax.broadcasted_iota(jnp.int32, (nr, nr), 1)
        cnt_lane = jnp.sum(jnp.where(sub == lane, cnt, 0.0), axis=0, keepdims=True)
        off = jnp.sum(jnp.where(lane < sub, cnt_lane, 0.0), axis=1, keepdims=True)
        index = jnp.where(masks == 1.0, ranks + off, float(vis_blk))
        cols_t = jnp.concatenate([index, jnp.zeros((128 - nr, 128), F32)], axis=0).T
        pick = lax.broadcasted_iota(jnp.int32, (tok, 128), 1)
        ZT[0:vis_blk, :] = Z[tb]
        ZT[vis_blk:128, :] = jnp.broadcast_to(mtok[...], (128 - vis_blk, dd))
        parts = []
        for q in range(per):
            column = jnp.sum(jnp.where(pick == dev0 + q, cols_t[0:tok, :], 0.0), axis=1, keepdims=True)
            one_hot = jnp.where(column == pick.astype(F32), 1.0, 0.0).astype(BF16)
            u = (mm(one_hot, ZT[...]) + DP[tb, dev0 + q].astype(F32)).astype(BF16)
            X1[pl.ds(pl.multiple_of(c * 256 + q * tok, tok), tok), dd:2 * dd] = u
            parts.append(norm(u, dvec[0, 0:1, :], dvec[1, 0:1, :]))
        HD[...] = jnp.concatenate(parts, axis=0)
        keys_values(0, HD[...], c)

    loop(ntok // 256, first_chunk)

    own = pl.ds(pl.multiple_of((t * nr + r) * tok, tok), tok)
    hidden = X1[own, dd:2 * dd]

    def dec_block(layer, hidden, normed):
        base = layer * d_w
        scale = float(dd // 16) ** -0.5 * LOG2E
        Q[0:tok, 0:dd] = (mm_t(normed, Z0[base:base + dd, 0:dd]) + dvec[4, layer:layer + 1, :]).astype(BF16)

        def group(g):
            cols = blk(g, 128)
            stacked = head_rows(Q[0:tok, cols], heads_g)

            def scores_of(c, top):
                sc = mm_t(X1[blk(c, 256), cols], stacked)
                S[blk(c, 256), :] = sc
                return jnp.maximum(top, jnp.max(sc, axis=0, keepdims=True))

            top = lax.fori_loop(0, ntok // 256, scores_of, jnp.full((1, heads_g * tok), -jnp.inf, F32))

            def probs_of(c, total):
                ex = jnp.exp2((S[blk(c, 256), :] - top) * scale)
                PR[blk(c, 256), :] = ex.astype(BF16)
                return total + jnp.sum(ex, axis=0, keepdims=True)

            total = lax.fori_loop(0, ntok // 256, probs_of, jnp.zeros((1, heads_g * tok), F32))
            out_t = mm(Y1[cols, 0:ntok], PR[...]) * (1.0 / total)
            ATT[0:tok, cols] = unstack_heads(out_t, heads_g).astype(BF16)

        loop(dd // 128, group)
        wo_rows = 2 * d_w + layer * dd
        acc = hidden.astype(F32) + mm(ATT[0:tok, 0:dd], Z0[wo_rows:wo_rows + dd, 0:dd]) + dvec[6, layer:layer + 1, :]
        resid = acc.astype(BF16)
        A[0:tok, 0:dd] = norm(resid, dvec[2, layer:layer + 1, :], dvec[3, layer:layer + 1, :])

        def up_cols(j):
            cols = blk(j, dd)
            up = mm(A[0:tok, 0:dd], Y0[layer * dd:(layer + 1) * dd, cols])
            HM[0:tok, cols] = gelu(up + dvec[8 + j, layer:layer + 1, :]).astype(BF16)

        loop(4, up_cols)
        down = mm(HM[0:tok, 0:4 * dd], Z0[layer * 4 * dd:(layer + 1) * 4 * dd, dd:2 * dd])
        return (resid.astype(F32) + down + dvec[7, layer:layer + 1, :]).astype(BF16)

    hidden = dec_block(0, hidden, norm(hidden, dvec[0, 0:1, :], dvec[1, 0:1, :]))
    A2[t, r] = norm(hidden, dvec[0, 1:2, :], dvec[1, 1:2, :])
    H1[0:tok, 0:dd] = hidden
    g2 = gather(A2, s_h, r_h)
    for step in g2[:4]:
        step()

    def second_chunk(c):
        tb = c // (nr // per)
        dev0 = lax.rem(c, nr // per) * per
        keys_values(1, A2[tb, pl.ds(dev0, per)].reshape(256, dd), c)

    loop(ntok // 256, second_chunk)
    hidden = dec_block(1, H1[0:tok, 0:dd], A2[t, r])
    out[...] = mm(norm(hidden, dfin[0:1, :], dfin[1:2, :]), Y0[0:dd, 4 * dd:4 * dd + w_out.shape[1]])

    for cp in st + fw + st2 + fw2 + stz:
        cp.wait_send()
    g1[4]()
    g2[4]()


def solution(mesh):
    nt, nr = mesh.shape["time"], mesh.shape["region"]

    def local_step(patches, enc_pos, vis_mask, dec_pos, w_embed, b_embed, enc_vec, enc_wqkv, enc_wo, enc_w1, enc_w2, enc_final, w_dec_in, mask_token, dec_vec, dec_wqkv, dec_wo, dec_w1, dec_w2, dec_final, w_out):
        tok = patches.shape[0]
        ed, dd = w_embed.shape[1], w_dec_in.shape[1]
        layers = enc_vec.shape[0]
        nvis = tok * nt * nr // KEEP_DIV
        ntok = tok * nt * nr
        flat = lambda w, width: jnp.transpose(w, (0, 2, 3, 4, 1)).reshape(layers, 3 * width, width)
        small = [patches, enc_pos, vis_mask.reshape(1, tok), dec_pos, b_embed.reshape(1, ed),
                 jnp.transpose(enc_vec, (1, 0, 2)), enc_final, mask_token.reshape(1, dd),
                 jnp.transpose(dec_vec, (1, 0, 2)), dec_final]
        big = [w_embed, flat(enc_wqkv, ed), enc_wo.reshape(layers, ed, ed), enc_w1, enc_w2, w_dec_in,
               flat(dec_wqkv, dd), dec_wo.reshape(layers, dd, dd), dec_w1, dec_w2, w_out]
        scratch = [
            pltpu.VMEM((4 * ed, ed), BF16), pltpu.VMEM((4 * ed, ed), BF16),
            pltpu.VMEM((ed, 4 * ed), BF16), pltpu.VMEM((ed, 4 * ed), BF16), pltpu.VMEM((4 * ed, ed), BF16),
            pltpu.VMEM((nr, tok // 2, ed), BF16), pltpu.VMEM((nr, 8, 128), F32), pltpu.VMEM((nt, nr, 128), F32),
            pltpu.VMEM((nvis, ed), BF16), pltpu.VMEM((nvis, ed), BF16), pltpu.VMEM((nvis, ed), BF16),
            pltpu.VMEM((nvis, ed), BF16), pltpu.VMEM((nvis, ed), BF16), pltpu.VMEM((nvis, ed), BF16),
            pltpu.VMEM((ed, nvis), BF16), pltpu.VMEM((nvis, ed), BF16), pltpu.VMEM((nvis, 4 * ed), BF16),
            pltpu.VMEM((nt, nvis // nt, dd), BF16), pltpu.VMEM((128, dd), BF16),
            pltpu.VMEM((nt, nr, tok, dd), BF16), pltpu.VMEM((nt, nr, tok, dd), BF16),
            pltpu.VMEM((ntok, 4 * tok), F32), pltpu.VMEM((ntok, 4 * tok), BF16), pltpu.VMEM((256, dd), BF16),
            pltpu.SemaphoreType.DMA((24,)),
            pltpu.SemaphoreType.DMA((64,)), pltpu.SemaphoreType.DMA((64,)),
            pltpu.SemaphoreType.DMA((64,)), pltpu.SemaphoreType.DMA((64,)),
            pltpu.SemaphoreType.DMA((64,)), pltpu.SemaphoreType.DMA((64,)),
        ]
        return pl.pallas_call(
            functools.partial(kernel, nt, nr),
            out_shape=jax.ShapeDtypeStruct((tok, w_out.shape[1]), F32),
            in_specs=[pl.BlockSpec(memory_space=pltpu.VMEM)] * len(small) + [pl.BlockSpec(memory_space=pl.ANY)] * len(big),
            out_specs=pl.BlockSpec(memory_space=pltpu.VMEM),
            scratch_shapes=scratch,
            compiler_params=pltpu.CompilerParams(collective_id=0, has_side_effects=True, vmem_limit_bytes=67043328),
            name="mae",
        )(*small, *big)

    token_rows = P(TOKEN_AXES, None)
    token_flags = P(TOKEN_AXES)
    replicated = P()
    in_specs = (token_rows, token_rows, token_flags, token_rows) + (replicated,) * 17
    return jax.shard_map(local_step, mesh=mesh, in_specs=in_specs, out_specs=token_rows, check_vma=False)
```

```python
import functools
import jax
import jax.numpy as jnp
from jax import lax
from jax.experimental import pallas as pl
from jax.experimental.pallas import tpu as pltpu
from jax.sharding import PartitionSpec as P

KEEP_DIV = 8
LN_EPS = 1e-6
CORES = 2
TOKEN_AXES = ("batch", "time", "region")
MESH_ID = pl.DeviceIdType.MESH
F32 = jnp.float32
BF16 = jnp.bfloat16
LOG2E = 1.4426950408889634


def mm(lhs, rhs):
    return jnp.dot(lhs, rhs, preferred_element_type=F32)


def mm_t(lhs, rhs):
    return lax.dot_general(lhs, rhs, (((1,), (1,)), ((), ())), preferred_element_type=F32)


def norm(rows, gain, shift):
    rows = rows.astype(F32)
    centered = rows - jnp.mean(rows, axis=-1, keepdims=True)
    variance = jnp.mean(centered * centered, axis=-1, keepdims=True)
    return (centered * lax.rsqrt(variance + LN_EPS) * gain + shift).astype(BF16)


def gelu(val):
    return 0.5 * val * (1.0 + lax.erf(val * 0.7071067811865476))


def loop(count, body):
    lax.fori_loop(0, count, lambda i, c: (body(i), c)[1], 0)


def blk(i, size):
    return pl.ds(pl.multiple_of(i * size, size), size)


def column_of(row, lanes):
    return jnp.broadcast_to(row, (lanes, row.shape[1])).T


def head_rows(q_rows, heads):
    lanes = q_rows.shape[1]
    head = iota(q_rows.shape, 1) // (lanes // heads)
    return jnp.concatenate([jnp.where(head == h, q_rows, jnp.zeros_like(q_rows)) for h in range(heads)], axis=0)


def unstack_heads(out_t, heads):
    out = out_t.T
    rows = out.shape[0] // heads
    head = iota((rows, out.shape[1]), 1) // (out.shape[1] // heads)
    total = jnp.where(head == 0, out[:rows], 0.0)
    for h in range(1, heads):
        total = total + jnp.where(head == h, out[h * rows:(h + 1) * rows], 0.0)
    return total


def rsum(val, axis):
    return jnp.sum(val, axis=axis, keepdims=True)


def rmax(val):
    return jnp.max(val, axis=0, keepdims=True)


def iota(shape, axis):
    return lax.broadcasted_iota(jnp.int32, shape, axis)


def kernel(nt, nr, count, *refs):
    given, refs = refs[:count], refs[count:]
    w_embed, wqkv, wo, w1, w2, w_dec, dqkv, dwo, dw1, dw2, out = refs[:11]
    held, refs = refs[11:11 + count], refs[11 + count:]
    (X0, X1, Y0, Y1, Z0, SS, SL, MT, MB, E, E2, H1, H2, A, Q, K, VT, ATT, HM, Z, IC, DP, A2, HD, QB, OT, ML,
     isem, wsem, s_e, r_e, s_g, r_g, s_h, r_h) = refs
    patches, enc_pos, vis, b_embed, dec_pos, evec, efin, mtok, dvec, dfin = held
    ld_in = [pltpu.make_async_copy(src, dst, isem.at[i]) for i, (src, dst) in enumerate(zip(given, held))]
    for cp in ld_in[2:3] + ld_in[:2]:
        cp.start()
    t = lax.axis_index("time")
    r = lax.axis_index("region")
    nx = nr // CORES
    x, core = r // CORES, lax.rem(r, CORES)
    partner = r + 1 - 2 * core
    tok = patches.shape[0]
    slots = SL.shape[1]
    vis_blk = E.shape[0] // nt
    ed, dd = E.shape[1], dec_pos.shape[1]
    nvis = E.shape[0]

    def xpeer(dx):
        return lax.rem(x + dx, nx) * CORES + core

    def tpeer(dy):
        return lax.rem(t + dy, nt)

    def xsrc(dx):
        return lax.rem(x + nx - dx, nx) * CORES + core

    def tsrc(dy):
        return lax.rem(t + nt - dy, nt)

    def rcopy(src, dst, ssem, rsem, tt, rr):
        return pltpu.make_async_remote_copy(src_ref=src, dst_ref=dst, send_sem=ssem, recv_sem=rsem,
                                            device_id={"time": tt, "region": rr}, device_id_type=MESH_ID)

    def load(src, dst, i):
        return pltpu.make_async_copy(src, dst, wsem.at[i])

    ld_embed = load(w_embed, Y1.at[:w_embed.shape[0], :ed], 0)
    ld_embed.start()
    for cp in ld_in[3:]:
        cp.start()

    barrier = pltpu.get_barrier_semaphore()
    order = [d for d in (1, 3, 2) if d < nx]
    across = [(t, partner, 1 - core)] + [(t, xpeer(d) + f * (1 - 2 * core), core + f * (1 - 2 * core)) for d in order for f in range(CORES)]
    peers = [p[:2] for p in across] + [(tpeer(d), r) for d in range(1, nt)]
    for tt, rr in peers:
        pl.semaphore_signal(barrier, inc=1, device_id={"time": tt, "region": rr}, device_id_type=MESH_ID)

    ld_in[2].wait()
    mask_row = vis[...].astype(F32)
    mask_pad = jnp.concatenate([mask_row, jnp.zeros((1, 128 - tok), F32)], axis=1)
    mask_pad = jnp.broadcast_to(mask_pad, (8, 128))
    MT[r] = mask_pad
    tri = (iota((128, 128), 0) < iota((128, 128), 1)).astype(BF16)
    local_rank = mm(mask_pad.astype(BF16), tri)[:1, :tok]
    selector = jnp.where((local_rank == iota((slots, tok), 0).astype(F32)) & (mask_row == 1.0), 1.0, 0.0).astype(BF16)
    for cp in ld_in[:2] + ld_in[3:]:
        cp.wait()

    ld_embed.wait()
    qkv_w, d_w = 3 * ed, 3 * dd
    ld_a = [load(wqkv.at[0], X0.at[:qkv_w], 1), load(wo.at[0], X0.at[qkv_w:qkv_w + ed], 2)]
    ld_b = [load(w1.at[0], Y0, 3), load(w2.at[0], Z0, 4)]
    ld_c = [load(wqkv.at[1], X1.at[:qkv_w], 5), load(wo.at[1], X1.at[qkv_w:qkv_w + ed], 6)]
    for cp in ld_a + ld_b + ld_c:
        cp.start()

    def embed_cols(j):
        cols = blk(j, 256)
        emb = (mm(patches[...], Y1[:patches.shape[1], cols]) + b_embed[:, cols] + enc_pos[:, cols].astype(F32)).astype(BF16)
        SS[j // 2, :, blk(lax.rem(j, 2), 256)] = mm(selector, emb).astype(BF16)

    loop(ed // 256, embed_cols)
    SL[r] = SS[core]
    ld_d = load(w1.at[1], Y1, 7)
    ld_d.start()
    token_row = jnp.broadcast_to(jnp.concatenate([mtok[i:i + 1, :] for i in range(dd // 128)], axis=1), (128 - vis_blk, dd))
    for tb in range(nt):
        Z[tb, vis_blk:128] = token_row
    pl.semaphore_wait(barrier, len(peers))

    st = []
    for i, (tt, rr, half) in enumerate(across):
        st.append(rcopy(SS.at[half], SL.at[r], s_e.at[i], r_e.at[i], tt, rr))
        st.append(rcopy(MT.at[r], MT.at[r], s_e.at[8 + i], r_e.at[8 + i], tt, rr))
    for cp in st:
        cp.start()
    sources = [partner] + [xsrc(d) + f * (1 - 2 * core) for d in order for f in range(CORES)]
    for i, src in enumerate(sources):
        rcopy(SL.at[src], SL.at[src], s_e.at[i], r_e.at[i], t, partner).wait_recv()
        rcopy(MT.at[src], MT.at[src], s_e.at[8 + i], r_e.at[8 + i], t, partner).wait_recv()

    mask_all = jnp.concatenate([MT[d, :1, :] for d in range(nr)], axis=0)
    MB[t] = mask_all
    counts = rsum(mask_all, 1)
    lane_dev = iota((nr, nr * slots), 1) // slots
    sub_dev = iota((nr, nr * slots), 0)
    lane_cnt = rsum(jnp.where(lane_dev == sub_dev, counts, 0.0), 0)
    lane_off = rsum(jnp.where(sub_dev < lane_dev, counts, 0.0), 0)
    lane_slot = lax.rem(iota((1, nr * slots), 1), slots).astype(F32)
    target = jnp.where(lane_slot < lane_cnt, lane_off + lane_slot, -1.0)
    rank_id = iota((vis_blk, nr * slots), 0).astype(F32)
    compact = jnp.where(target == rank_id, 1.0, 0.0).astype(BF16)
    my_rows = blk(t, vis_blk)

    eh = ed // CORES
    my_cols, other_cols = blk(core, eh), blk(1 - core, eh)
    E[my_rows, my_cols] = mm(compact, SL[...].reshape(nr * slots, eh)).astype(BF16)

    mine = E.at[my_rows, my_cols]
    st2 = []
    for d in range(1, nt):
        st2.append(rcopy(mine, mine, s_e.at[32 + d], r_e.at[32 + d], tpeer(d), r))
        st2.append(rcopy(MB.at[t], MB.at[t], s_e.at[40 + d], r_e.at[40 + d], tpeer(d), r))
    st2.append(rcopy(mine, mine, s_e.at[48], r_e.at[48], t, partner))
    for cp in st2:
        cp.start()
    DP[t, r] = dec_pos[...]

    def gather(buf, ss, rs):
        hw = dd // 2
        first, second, third = [], [], {}

        def step1():
            own = buf.at[t, r]
            for d in order:
                first.append(rcopy(own, own, ss.at[d], rs.at[d], tpeer(d), r))
                first.append(rcopy(own, own, ss.at[4 + d], rs.at[4 + d], t, xpeer(d)))
            first.append(rcopy(own, own, ss.at[0], rs.at[0], t, partner))
            for cp in first:
                cp.start()

        def to_partner(ref, d, e):
            i = 40 + d * 4 + e
            cp = rcopy(ref, ref, ss.at[i], rs.at[i], t, partner)
            cp.start()
            third[(d, e)] = cp

        def step2(d):
            src = tsrc(d)
            rcopy(buf.at[src, r], buf.at[src, r], ss.at[d], rs.at[d], t, partner).wait_recv()
            for e in range(1, nx):
                i = 8 + d * 4 + e
                low = buf.at[src, r, :, :hw]
                second.append(rcopy(low, low, ss.at[i], rs.at[i], t, xpeer(e)))
                second[-1].start()
            to_partner(buf.at[src, r], d, 0)
            src = xsrc(d)
            rcopy(buf.at[t, src], buf.at[t, src], ss.at[4 + d], rs.at[4 + d], t, partner).wait_recv()
            for e in range(1, nt):
                i = 24 + d * 4 + e
                high = buf.at[t, src, :, hw:]
                second.append(rcopy(high, high, ss.at[i], rs.at[i], tpeer(e), r))
                second[-1].start()
            to_partner(buf.at[t, src], 0, d)

        def step3(d, e):
            ref = buf.at[tsrc(d), xsrc(e)]
            low, high = ref.at[:, :hw], ref.at[:, hw:]
            rcopy(low, low, ss.at[8 + d * 4 + e], rs.at[8 + d * 4 + e], t, partner).wait_recv()
            rcopy(high, high, ss.at[24 + e * 4 + d], rs.at[24 + e * 4 + d], t, partner).wait_recv()
            to_partner(ref, d, e)

        def finish(d, e):
            if d == 0 and e == 0:
                rcopy(buf.at[t, partner], buf.at[t, partner], ss.at[0], rs.at[0], t, partner).wait_recv()
            else:
                third[(d, e)].wait_recv()

        def drain():
            for cp in first + second + list(third.values()):
                cp.wait_send()

        return step1, step2, step3, finish, drain

    g1 = gather(DP, s_g, r_g)
    g1[0]()

    def index_cols(masks):
        ranks = mm(masks.astype(BF16), tri)
        sub, lane = iota((nr, nr), 0), iota((nr, nr), 1)
        cnt_lane = rsum(jnp.where(sub == lane, rsum(masks, 1), 0.0), 0)
        off = rsum(jnp.where(lane < sub, cnt_lane, 0.0), 1)
        index = jnp.where(masks == 1.0, ranks + off, float(vis_blk))
        return jnp.concatenate([index, jnp.zeros((128 - nr, 128), F32)], axis=0).T

    def norm_rows(src, dst, count, gain, shift, start, dst_start, step=64):
        def body(i):
            rows = pl.ds(pl.multiple_of(start + i * step, step), step)
            dst[pl.ds(pl.multiple_of(dst_start + i * step, step), step), :] = norm(src[rows, :], gain, shift)
        loop(count // step, body)

    fw2 = []

    def rows0(vec):
        def take(block, i):
            got = E.at[blk(block, vis_blk), other_cols]
            rcopy(got, got, s_e.at[48 + i], r_e.at[48 + i], t, partner).wait_recv()
            norm_rows(E, A, vis_blk, vec(0), vec(1), block * vis_blk, block * vis_blk)

        take(t, 0)
        for d in order:
            got = E.at[blk(tsrc(d), vis_blk), my_cols]
            rcopy(got, got, s_e.at[32 + d], r_e.at[32 + d], t, partner).wait_recv()
            fw2.append(rcopy(got, got, s_e.at[48 + d], r_e.at[48 + d], t, partner))
            fw2[-1].start()
            rcopy(MB.at[tsrc(d)], MB.at[tsrc(d)], s_e.at[40 + d], r_e.at[40 + d], t, partner).wait_recv()
        for d in order:
            take(tsrc(d), d)

    def project(dst, rows_n, src_rows, w, w_row, bias):
        def body(j):
            cols = blk(j, 512)
            acc = mm_t(A[src_rows, :], w[pl.ds(pl.multiple_of(w_row + j * 512, 512), 512), :])
            if bias is not None:
                acc = acc + bias(cols)
            dst[:rows_n, cols] = acc.astype(BF16)
        loop(ed // 512, body)

    def enc_layer(layer, w_a, w_up, w_down, src, dst, rows_n, start, dst_start, pairs, wait_rows, wait_down):
        def vec(i):
            return evec[i, layer:layer + 1, :]

        wait_rows(vec)
        q_rows = pl.ds(pl.multiple_of(start, rows_n), rows_n)
        project(Q, rows_n, q_rows, w_a, 0, lambda cols: evec[4, layer:layer + 1, cols])
        project(K, nvis, slice(None), w_a, ed, None)

        def v_rows(j):
            rows = blk(j, 512)
            bias = column_of(evec[5, layer:layer + 1, rows], 128)
            acc = mm_t(w_a[pl.ds(pl.multiple_of(2 * ed + j * 512, 512), 512), :], A[...])
            VT[rows, :] = (acc + jnp.concatenate([bias] * (nvis // 128), axis=1)).astype(BF16)

        loop(ed // 512, v_rows)

        def heads2(p):
            for q in range(pairs):
                cols = blk(p * pairs + q, 128)
                scores = mm_t(K[:, cols], head_rows(Q[:rows_n, cols], 2))
                top = rmax(scores)
                ex = jnp.exp2((scores - top) * (0.125 * LOG2E))
                prob = (ex * (1.0 / rsum(ex, 0))).astype(BF16)
                ATT[:rows_n, cols] = unstack_heads(mm(VT[cols, :], prob), 2).astype(BF16)

        loop(ed // 128 // pairs, heads2)

        def out_cols(j):
            cols = blk(j, 512)
            acc = src[q_rows, cols].astype(F32) + mm(ATT[:rows_n, :], w_a[3 * ed:4 * ed, cols])
            H1[:rows_n, cols] = (acc + evec[6, layer:layer + 1, cols]).astype(BF16)

        loop(ed // 512, out_cols)
        wait_down()
        norm_rows(H1, A, rows_n, vec(2), vec(3), 0, 0)

        def up_cols(j):
            acc = mm(A[:rows_n, :], w_up[:, blk(j, ed)])
            HM[:rows_n, blk(j, ed)] = gelu(acc + evec[8 + j, layer:layer + 1, :]).astype(BF16)

        loop(w_up.shape[1] // ed, up_cols)
        o_rows = pl.ds(pl.multiple_of(dst_start, rows_n), rows_n)

        def down_cols(j):
            cols = blk(j, 256)
            acc = H1[:rows_n, cols].astype(F32) + mm(HM[:rows_n, :], w_down[:, cols])
            dst[o_rows, cols] = (acc + evec[7, layer:layer + 1, cols]).astype(BF16)

        loop(ed // 256, down_cols)

    for cp in ld_a:
        cp.wait()
    ld_e = load(w2.at[1], X0, 8)

    def mid0():
        ld_e.start()
        for d in order:
            g1[1](d)
        for cp in ld_b:
            cp.wait()

    hv = nvis // CORES
    enc_layer(0, X0, Y0, Z0, E, H2, hv, core * hv, core * hv, 2,
              rows0, mid0)
    h_mine = pl.ds(pl.multiple_of(core * hv, hv), hv)
    swap = rcopy(H2.at[h_mine], H2.at[h_mine], s_e.at[60], r_e.at[60], t, partner)
    swap.start()
    dh = w_dec.shape[0]
    ld_f = []
    for l in range(2):
        ld_f.append(load(dqkv.at[l], Z0.at[l * d_w:(l + 1) * d_w, :dd], 9 + l))
        ld_f.append(load(dwo.at[l], Z0.at[2 * d_w + l * dd:2 * d_w + (l + 1) * dd, :dd], 11 + l))
        ld_f.append(load(dw1.at[l], Y0.at[l * dd:(l + 1) * dd, :4 * dd], 13 + l))
        ld_f.append(load(dw2.at[l], Z0.at[l * 4 * dd:(l + 1) * 4 * dd, dd:2 * dd], 15 + l))
    ld_dec = load(w_dec, Y0.at[:dh, 6 * dd:7 * dd], 18)
    ld_dec.start()
    for cp in ld_f:
        cp.start()
    for cp in ld_c:
        cp.wait()

    def mid1():
        for d in order:
            for e in order:
                g1[2](d, e)
        ld_d.wait()
        ld_e.wait()

    def rows1(vec):
        norm_rows(H2, A, hv, vec(0), vec(1), core * hv, core * hv)
        other = pl.ds(pl.multiple_of((1 - core) * hv, hv), hv)
        rcopy(H2.at[other], H2.at[other], s_e.at[60], r_e.at[60], t, partner).wait_recv()
        norm_rows(H2, A, hv, vec(0), vec(1), (1 - core) * hv, (1 - core) * hv)

    enc_layer(1, X1, Y1, X0, H2, E2, vis_blk, t * vis_blk, 0, 4, rows1, mid1)
    norm_rows(E2, A, vis_blk, efin[:1, :], efin[1:2, :], 0, 0)
    ld_dec.wait()
    z_mine = Z.at[t, :vis_blk]
    Z[t, :vis_blk] = mm(A[:vis_blk, :], Y0[:dh, 6 * dd:7 * dd]).astype(BF16)
    stz = []
    for d in range(1, nt):
        stz.append(rcopy(z_mine, z_mine, s_e.at[56 + d], r_e.at[56 + d], tpeer(d), r))
    for cp in stz:
        cp.start()
    for tb in range(nt):
        IC[tb] = index_cols(MB[tb])
    for d in range(nt):
        for e in range(nx):
            g1[3](d, e)
    for cp in ld_f:
        cp.wait()

    groups = dd // 128
    heads_g = 4
    stack = heads_g * tok
    scale = float(dd // (groups * heads_g)) ** -0.5 * LOG2E
    blk_tok = nr * tok

    pick = iota((tok, 128), 1)

    def one_hot(column):
        return jnp.where(column == pick.astype(F32), 1.0, 0.0).astype(BF16)

    own_col = rsum(jnp.where(pick == r, IC[t, :tok, :], 0.0), 1)
    hidden = (mm(one_hot(own_col), Z[t]) + DP[t, r].astype(F32)).astype(BF16)

    def start_attention(layer, normed):
        base = layer * d_w
        q_all = (mm_t(normed, Z0[base:base + dd, :dd]) + dvec[4, layer:layer + 1, :]).astype(BF16)
        for g in range(groups):
            QB[g] = head_rows(q_all[:, g * 128:(g + 1) * 128], heads_g)
        OT[...] = jnp.zeros(OT.shape, F32)
        ML[:groups] = jnp.full((groups, 1, stack), -jnp.inf, F32)
        ML[groups:2 * groups] = jnp.zeros((groups, 1, stack), F32)

    def attend(layer, rows):
        base = layer * d_w
        keys = mm_t(rows, Z0[base + dd:base + 2 * dd, :dd]).astype(BF16)
        acc = mm_t(Z0[base + 2 * dd:base + 3 * dd, :dd], rows)
        bias = column_of(dvec[5, layer:layer + 1, :], 128)
        values = (acc + jnp.concatenate([bias] * (rows.shape[0] // 128), axis=1)).astype(BF16)
        for g in range(groups):
            sc = mm_t(keys[:, g * 128:(g + 1) * 128], QB[g])
            old = ML[g]
            top = jnp.maximum(old, rmax(sc))
            ex = jnp.exp2((sc - top) * scale)
            keep = jnp.exp2((old - top) * scale)
            ML[g] = top
            ML[groups + g] = ML[groups + g] * keep + rsum(ex, 0)
            lanes = slice(g * 128, (g + 1) * 128)
            OT[lanes, :] = OT[lanes, :] * keep + mm(values[lanes, :], ex.astype(BF16))

    def finish_block(layer, hidden):
        for g in range(groups):
            lanes = slice(g * 128, (g + 1) * 128)
            ATT[:tok, lanes] = unstack_heads(OT[lanes, :] * (1.0 / ML[groups + g]), heads_g).astype(BF16)
        wo_rows = 2 * d_w + layer * dd
        acc = hidden.astype(F32) + mm(ATT[:tok, :dd], Z0[wo_rows:wo_rows + dd, :dd]) + dvec[6, layer:layer + 1, :]
        resid = acc.astype(BF16)
        normed = norm(resid, dvec[2, layer:layer + 1, :], dvec[3, layer:layer + 1, :])
        for j in range(4):
            cols = slice(j * dd, (j + 1) * dd)
            up = mm(normed, Y0[layer * dd:(layer + 1) * dd, cols])
            HM[:tok, cols] = gelu(up + dvec[8 + j, layer:layer + 1, :]).astype(BF16)
        down = mm(HM[:tok, :4 * dd], Z0[layer * 4 * dd:(layer + 1) * 4 * dd, dd:2 * dd])
        return (resid.astype(F32) + down + dvec[7, layer:layer + 1, :]).astype(BF16)

    start_attention(0, norm(hidden, dvec[0, :1, :], dvec[1, :1, :]))

    def first_unit(d):
        tb = lax.rem(t + nt - d, nt)
        cols_t = IC[tb]

        @pl.when(d > 0)
        def _():
            ref = Z.at[tb, :vis_blk]
            rcopy(ref, ref, s_e.at[56 + d], r_e.at[56 + d], t, r).wait_recv()

        for q in range(nr):
            u = (mm(one_hot(cols_t[:tok, q:q + 1]), Z[tb]) + DP[tb, q].astype(F32)).astype(BF16)
            HD[q * tok:(q + 1) * tok, :] = norm(u, dvec[0, :1, :], dvec[1, :1, :])
        attend(0, HD[...])

    loop(nt, first_unit)
    hidden = finish_block(0, hidden)
    A2[t, r] = norm(hidden, dvec[0, 1:2, :], dvec[1, 1:2, :])
    H1[:tok, :dd] = hidden
    g2 = gather(A2, s_h, r_h)
    g2[0]()
    start_attention(1, A2[t, r])

    def unit(*chips):
        parts = []
        for d, e in chips:
            g2[3](d, e)
            xs = lax.rem(x + nx - e, nx) * CORES
            parts.append(A2[tsrc(d), pl.ds(xs, CORES)].reshape(CORES * tok, dd))
        attend(1, jnp.concatenate(parts, axis=0))

    g2[1](1)
    g2[1](3)
    unit((0, 0), (1, 0), (3, 0), (0, 1))
    g2[1](2)
    unit((0, 3), (2, 0), (0, 2))
    near = [(1, 1), (1, 3), (3, 1), (3, 3)]
    far = [(1, 2), (2, 1), (2, 3), (3, 2)]
    for d, e in near + far:
        g2[2](d, e)
    unit(*near)
    g2[2](2, 2)
    unit(*far, (2, 2))
    hidden = finish_block(1, H1[:tok, :dd])
    out[...] = norm(hidden, dfin[:1, :], dfin[1:2, :])

    for cp in st + st2 + fw2 + stz + [swap]:
        cp.wait_send()
    g1[4]()
    g2[4]()


def solution(mesh):
    nt, nr = mesh.shape["time"], mesh.shape["region"]

    def local_step(patches, enc_pos, vis_mask, dec_pos, w_embed, b_embed, enc_vec, enc_wqkv, enc_wo, enc_w1, enc_w2, enc_final, w_dec_in, mask_token, dec_vec, dec_wqkv, dec_wo, dec_w1, dec_w2, dec_final, w_out):
        tok = patches.shape[0]
        ed, dd = w_embed.shape[1], w_dec_in.shape[1]
        layers = enc_vec.shape[0]
        nvis = tok * nt * nr // KEEP_DIV
        flat = lambda w, width: jnp.transpose(w, (0, 2, 3, 4, 1)).reshape(layers, 3 * width, width)
        small = [patches, enc_pos, vis_mask.reshape(1, tok), b_embed.reshape(1, ed), dec_pos,
                 jnp.transpose(enc_vec, (1, 0, 2)), enc_final, mask_token.reshape(dd // 128, 128),
                 jnp.transpose(dec_vec, (1, 0, 2)), dec_final]
        big = [w_embed, flat(enc_wqkv, ed), enc_wo.reshape(layers, ed, ed), enc_w1, enc_w2, w_dec_in,
               flat(dec_wqkv, dd), dec_wo.reshape(layers, dd, dd), dec_w1, dec_w2]
        scratch = [pltpu.VMEM(v.shape, v.dtype) for v in small] + [
            pltpu.VMEM((4 * ed, ed), BF16), pltpu.VMEM((4 * ed, ed), BF16),
            pltpu.VMEM((ed, 4 * ed), BF16), pltpu.VMEM((ed, 4 * ed), BF16), pltpu.VMEM((4 * ed, ed), BF16),
            pltpu.VMEM((CORES, tok // 2, ed // CORES), BF16), pltpu.VMEM((nr, tok // 2, ed // CORES), BF16), pltpu.VMEM((nr, 8, 128), F32), pltpu.VMEM((nt, nr, 128), F32),
            pltpu.VMEM((nvis, ed), BF16), pltpu.VMEM((nvis // nt, ed), BF16), pltpu.VMEM((nvis // CORES, ed), BF16), pltpu.VMEM((nvis, ed), BF16),
            pltpu.VMEM((nvis, ed), BF16), pltpu.VMEM((nvis // CORES, ed), BF16), pltpu.VMEM((nvis, ed), BF16),
            pltpu.VMEM((ed, nvis), BF16), pltpu.VMEM((nvis // CORES, ed), BF16), pltpu.VMEM((nvis // CORES, 4 * ed), BF16),
            pltpu.VMEM((nt, 128, dd), BF16), pltpu.VMEM((nt, 128, 128), F32),
            pltpu.VMEM((nt, nr, tok, dd), BF16), pltpu.VMEM((nt, nr, tok, dd), BF16),
            pltpu.VMEM((nr * tok, dd), BF16), pltpu.VMEM((dd // 128, 4 * tok, 128), BF16),
            pltpu.VMEM((dd, 4 * tok), F32), pltpu.VMEM((2 * dd // 128, 1, 4 * tok), F32),
        ] + [pltpu.SemaphoreType.DMA((n,)) for n in (16, 24) + (64,) * 6]
        rows = pl.pallas_call(
            functools.partial(kernel, nt, nr, len(small)),
            out_shape=jax.ShapeDtypeStruct((tok, dd), BF16),
            in_specs=[pl.BlockSpec(memory_space=pl.ANY)] * (len(small) + len(big)),
            out_specs=pl.BlockSpec(memory_space=pltpu.VMEM),
            scratch_shapes=scratch,
            compiler_params=pltpu.CompilerParams(collective_id=0, has_side_effects=True, vmem_limit_bytes=64 * 1024 * 1024 - 65536),
            name="mae",
        )(*small, *big)
        return mm(rows, w_out)

    token_rows = P(TOKEN_AXES, None)
    token_flags = P(TOKEN_AXES)
    replicated = P()
    in_specs = (token_rows, token_rows, token_flags, token_rows) + (replicated,) * 17
    return jax.shard_map(local_step, mesh=mesh, in_specs=in_specs, out_specs=token_rows, check_vma=False)
```

```python
import functools
import jax
import jax.numpy as jnp
from jax import lax
from jax.experimental import pallas as pl
from jax.experimental.pallas import tpu as pltpu
from jax.sharding import PartitionSpec as P

KEEP_DIV = 8
LN_EPS = 1e-6
CORES = 2
TOKEN_AXES = ("batch", "time", "region")
MESH_ID = pl.DeviceIdType.MESH
F32 = jnp.float32
BF16 = jnp.bfloat16
LOG2E = 1.4426950408889634


def mm(lhs, rhs):
    return jnp.dot(lhs, rhs, preferred_element_type=F32)


def mm_t(lhs, rhs):
    return lax.dot_general(lhs, rhs, (((1,), (1,)), ((), ())), preferred_element_type=F32)


def norm(rows, gain, shift):
    rows = rows.astype(F32)
    centered = rows - jnp.mean(rows, axis=-1, keepdims=True)
    variance = jnp.mean(centered * centered, axis=-1, keepdims=True)
    return (centered * lax.rsqrt(variance + LN_EPS) * gain + shift).astype(BF16)


def gelu(val):
    return 0.5 * val * (1.0 + lax.erf(val * 0.7071067811865476))


def loop(count, body):
    lax.fori_loop(0, count, lambda i, c: (body(i), c)[1], 0)


def blk(i, size):
    return pl.ds(pl.multiple_of(i * size, size), size)


def column_of(row, lanes):
    return jnp.broadcast_to(row, (lanes, row.shape[1])).T


def head_rows(q_rows, heads):
    lanes = q_rows.shape[1]
    head = iota(q_rows.shape, 1) // (lanes // heads)
    return jnp.concatenate([jnp.where(head == h, q_rows, jnp.zeros_like(q_rows)) for h in range(heads)], axis=0)


def unstack_heads(out_t, heads):
    out = out_t.T
    rows = out.shape[0] // heads
    head = iota((rows, out.shape[1]), 1) // (out.shape[1] // heads)
    total = jnp.where(head == 0, out[:rows], 0.0)
    for h in range(1, heads):
        total = total + jnp.where(head == h, out[h * rows:(h + 1) * rows], 0.0)
    return total


def rsum(val, axis):
    return jnp.sum(val, axis=axis, keepdims=True)


def rmax(val):
    return jnp.max(val, axis=0, keepdims=True)


def iota(shape, axis):
    return lax.broadcasted_iota(jnp.int32, shape, axis)


def kernel(nt, nr, count, *refs):
    given, refs = refs[:count], refs[count:]
    w_embed, wqkv, wo, w1, w2, w_dec, dqkv, dwo, dw1, dw2, out = refs[:11]
    held, refs = refs[11:11 + count], refs[11 + count:]
    (X0, X1, Y0, Y1, Z0, SS, SL, MT, MB, E, E2, H1, H2, A, Q, K, VT, ATT, HM, Z, IC, DP, A2, HD, QB, OT, ML,
     isem, wsem, s_e, r_e, s_g, r_g, s_h, r_h) = refs
    patches, enc_pos, vis, b_embed, dec_pos, evec, efin, mtok, dvec, dfin = held
    ld_in = [pltpu.make_async_copy(src, dst, isem.at[i]) for i, (src, dst) in enumerate(zip(given, held))]
    for cp in ld_in[2:3] + ld_in[:2]:
        cp.start()
    t = lax.axis_index("time")
    r = lax.axis_index("region")
    nx = nr // CORES
    x, core = r // CORES, lax.rem(r, CORES)
    partner = r + 1 - 2 * core
    tok = patches.shape[0]
    slots = SL.shape[1]
    vis_blk = E.shape[0] // nt
    ed, dd = E.shape[1], dec_pos.shape[1]
    nvis = E.shape[0]

    def xpeer(dx):
        return lax.rem(x + dx, nx) * CORES + core

    def tpeer(dy):
        return lax.rem(t + dy, nt)

    def xsrc(dx):
        return lax.rem(x + nx - dx, nx) * CORES + core

    def tsrc(dy):
        return lax.rem(t + nt - dy, nt)

    def rcopy(src, dst, ssem, rsem, tt, rr):
        return pltpu.make_async_remote_copy(src_ref=src, dst_ref=dst, send_sem=ssem, recv_sem=rsem,
                                            device_id={"time": tt, "region": rr}, device_id_type=MESH_ID)

    def load(src, dst, i):
        return pltpu.make_async_copy(src, dst, wsem.at[i])

    ld_embed = load(w_embed, Y1.at[:w_embed.shape[0], :ed], 0)
    ld_embed.start()
    for cp in ld_in[3:]:
        cp.start()

    barrier = pltpu.get_barrier_semaphore()
    order = [d for d in (1, 3, 2) if d < nx]
    across = [(t, partner, 1 - core)] + [(t, xpeer(d) + f * (1 - 2 * core), core + f * (1 - 2 * core)) for d in order for f in range(CORES)]
    peers = [p[:2] for p in across] + [(tpeer(d), r) for d in range(1, nt)]
    for tt, rr in peers:
        pl.semaphore_signal(barrier, inc=1, device_id={"time": tt, "region": rr}, device_id_type=MESH_ID)

    ld_in[2].wait()
    mask_row = vis[...].astype(F32)
    mask_pad = jnp.concatenate([mask_row, jnp.zeros((1, 128 - tok), F32)], axis=1)
    mask_pad = jnp.broadcast_to(mask_pad, (8, 128))
    MT[r] = mask_pad
    tri = (iota((128, 128), 0) < iota((128, 128), 1)).astype(BF16)
    local_rank = mm(mask_pad.astype(BF16), tri)[:1, :tok]
    selector = jnp.where((local_rank == iota((slots, tok), 0).astype(F32)) & (mask_row == 1.0), 1.0, 0.0).astype(BF16)
    for cp in ld_in[:2] + ld_in[3:]:
        cp.wait()

    ld_embed.wait()
    qkv_w, d_w = 3 * ed, 3 * dd
    ld_a = [load(wqkv.at[0], X0.at[:qkv_w], 1), load(wo.at[0], X0.at[qkv_w:qkv_w + ed], 2)]
    ld_b = [load(w1.at[0], Y0, 3), load(w2.at[0], Z0, 4)]
    ld_c = [load(wqkv.at[1], X1.at[:qkv_w], 5), load(wo.at[1], X1.at[qkv_w:qkv_w + ed], 6)]
    for cp in ld_a + ld_b + ld_c:
        cp.start()

    def embed_cols(j):
        cols = blk(j, 256)
        emb = (mm(patches[...], Y1[:patches.shape[1], cols]) + b_embed[:, cols] + enc_pos[:, cols].astype(F32)).astype(BF16)
        SS[j // 2, :, blk(lax.rem(j, 2), 256)] = mm(selector, emb).astype(BF16)

    loop(ed // 256, embed_cols)
    SL[r] = SS[core]
    ld_d = load(w1.at[1], Y1, 7)
    ld_d.start()
    token_row = jnp.broadcast_to(jnp.concatenate([mtok[i:i + 1, :] for i in range(dd // 128)], axis=1), (128 - vis_blk, dd))
    for tb in range(nt):
        Z[tb, vis_blk:128] = token_row
    pl.semaphore_wait(barrier, len(peers))

    st = []
    for i, (tt, rr, half) in enumerate(across):
        st.append(rcopy(SS.at[half], SL.at[r], s_e.at[i], r_e.at[i], tt, rr))
        st.append(rcopy(MT.at[r], MT.at[r], s_e.at[8 + i], r_e.at[8 + i], tt, rr))
    for cp in st:
        cp.start()
    sources = [partner] + [xsrc(d) + f * (1 - 2 * core) for d in order for f in range(CORES)]
    for i, src in enumerate(sources):
        rcopy(SL.at[src], SL.at[src], s_e.at[i], r_e.at[i], t, partner).wait_recv()
        rcopy(MT.at[src], MT.at[src], s_e.at[8 + i], r_e.at[8 + i], t, partner).wait_recv()

    mask_all = jnp.concatenate([MT[d, :1, :] for d in range(nr)], axis=0)
    MB[t] = mask_all
    counts = rsum(mask_all, 1)
    lane_dev = iota((nr, nr * slots), 1) // slots
    sub_dev = iota((nr, nr * slots), 0)
    lane_cnt = rsum(jnp.where(lane_dev == sub_dev, counts, 0.0), 0)
    lane_off = rsum(jnp.where(sub_dev < lane_dev, counts, 0.0), 0)
    lane_slot = lax.rem(iota((1, nr * slots), 1), slots).astype(F32)
    target = jnp.where(lane_slot < lane_cnt, lane_off + lane_slot, -1.0)
    rank_id = iota((vis_blk, nr * slots), 0).astype(F32)
    compact = jnp.where(target == rank_id, 1.0, 0.0).astype(BF16)
    my_rows = blk(t, vis_blk)

    eh = ed // CORES
    my_cols, other_cols = blk(core, eh), blk(1 - core, eh)
    E[my_rows, my_cols] = mm(compact, SL[...].reshape(nr * slots, eh)).astype(BF16)

    mine = E.at[my_rows, my_cols]
    st2 = []
    for d in range(1, nt):
        st2.append(rcopy(mine, mine, s_e.at[32 + d], r_e.at[32 + d], tpeer(d), r))
        st2.append(rcopy(MB.at[t], MB.at[t], s_e.at[40 + d], r_e.at[40 + d], tpeer(d), r))
    st2.append(rcopy(mine, mine, s_e.at[48], r_e.at[48], t, partner))
    for cp in st2:
        cp.start()
    DP[t, r] = dec_pos[...]

    def gather(buf, ss, rs):
        hw = dd // 2
        first, second, third = [], [], {}

        def step1():
            own = buf.at[t, r]
            for d in order:
                first.append(rcopy(own, own, ss.at[d], rs.at[d], tpeer(d), r))
                first.append(rcopy(own, own, ss.at[4 + d], rs.at[4 + d], t, xpeer(d)))
            first.append(rcopy(own, own, ss.at[0], rs.at[0], t, partner))
            for cp in first:
                cp.start()

        def to_partner(ref, d, e):
            i = 40 + d * 4 + e
            cp = rcopy(ref, ref, ss.at[i], rs.at[i], t, partner)
            cp.start()
            third[(d, e)] = cp

        def step2(d):
            src = tsrc(d)
            rcopy(buf.at[src, r], buf.at[src, r], ss.at[d], rs.at[d], t, partner).wait_recv()
            for e in range(1, nx):
                i = 8 + d * 4 + e
                low = buf.at[src, r, :, :hw]
                second.append(rcopy(low, low, ss.at[i], rs.at[i], t, xpeer(e)))
                second[-1].start()
            to_partner(buf.at[src, r], d, 0)
            src = xsrc(d)
            rcopy(buf.at[t, src], buf.at[t, src], ss.at[4 + d], rs.at[4 + d], t, partner).wait_recv()
            for e in range(1, nt):
                i = 24 + d * 4 + e
                high = buf.at[t, src, :, hw:]
                second.append(rcopy(high, high, ss.at[i], rs.at[i], tpeer(e), r))
                second[-1].start()
            to_partner(buf.at[t, src], 0, d)

        def step3(d, e):
            ref = buf.at[tsrc(d), xsrc(e)]
            low, high = ref.at[:, :hw], ref.at[:, hw:]
            rcopy(low, low, ss.at[8 + d * 4 + e], rs.at[8 + d * 4 + e], t, partner).wait_recv()
            rcopy(high, high, ss.at[24 + e * 4 + d], rs.at[24 + e * 4 + d], t, partner).wait_recv()
            to_partner(ref, d, e)

        def finish(d, e):
            if d == 0 and e == 0:
                rcopy(buf.at[t, partner], buf.at[t, partner], ss.at[0], rs.at[0], t, partner).wait_recv()
            else:
                third[(d, e)].wait_recv()

        def drain():
            for cp in first + second + list(third.values()):
                cp.wait_send()

        return step1, step2, step3, finish, drain

    g1 = gather(DP, s_g, r_g)
    g1[0]()

    def index_cols(masks):
        ranks = mm(masks.astype(BF16), tri)
        sub, lane = iota((nr, nr), 0), iota((nr, nr), 1)
        cnt_lane = rsum(jnp.where(sub == lane, rsum(masks, 1), 0.0), 0)
        off = rsum(jnp.where(lane < sub, cnt_lane, 0.0), 1)
        index = jnp.where(masks == 1.0, ranks + off, float(vis_blk))
        return jnp.concatenate([index, jnp.zeros((128 - nr, 128), F32)], axis=0).T

    def norm_rows(src, dst, count, gain, shift, start, dst_start, step=64):
        def body(i):
            rows = pl.ds(pl.multiple_of(start + i * step, step), step)
            dst[pl.ds(pl.multiple_of(dst_start + i * step, step), step), :] = norm(src[rows, :], gain, shift)
        loop(count // step, body)

    fw2 = []

    def rows0(vec):
        def take(block, i):
            got = E.at[blk(block, vis_blk), other_cols]
            rcopy(got, got, s_e.at[48 + i], r_e.at[48 + i], t, partner).wait_recv()
            norm_rows(E, A, vis_blk, vec(0), vec(1), block * vis_blk, block * vis_blk)

        take(t, 0)
        for d in order:
            got = E.at[blk(tsrc(d), vis_blk), my_cols]
            rcopy(got, got, s_e.at[32 + d], r_e.at[32 + d], t, partner).wait_recv()
            fw2.append(rcopy(got, got, s_e.at[48 + d], r_e.at[48 + d], t, partner))
            fw2[-1].start()
            rcopy(MB.at[tsrc(d)], MB.at[tsrc(d)], s_e.at[40 + d], r_e.at[40 + d], t, partner).wait_recv()
        for d in order:
            take(tsrc(d), d)

    def project(dst, rows_n, src_rows, w, w_row, bias):
        def body(j):
            cols = blk(j, 512)
            acc = mm_t(A[src_rows, :], w[pl.ds(pl.multiple_of(w_row + j * 512, 512), 512), :])
            if bias is not None:
                acc = acc + bias(cols)
            dst[:rows_n, cols] = acc.astype(BF16)
        loop(ed // 512, body)

    def enc_layer(layer, w_a, w_up, w_down, src, dst, rows_n, start, dst_start, pairs, wait_rows, wait_down):
        def vec(i):
            return evec[i, layer:layer + 1, :]

        wait_rows(vec)
        q_rows = pl.ds(pl.multiple_of(start, rows_n), rows_n)
        project(Q, rows_n, q_rows, w_a, 0, lambda cols: evec[4, layer:layer + 1, cols])
        project(K, nvis, slice(None), w_a, ed, None)

        def v_rows(j):
            rows = blk(j, 512)
            bias = column_of(evec[5, layer:layer + 1, rows], 128)
            acc = mm_t(w_a[pl.ds(pl.multiple_of(2 * ed + j * 512, 512), 512), :], A[...])
            VT[rows, :] = (acc + jnp.concatenate([bias] * (nvis // 128), axis=1)).astype(BF16)

        loop(ed // 512, v_rows)

        def heads2(p):
            for q in range(pairs):
                cols = blk(p * pairs + q, 128)
                scores = mm_t(K[:, cols], head_rows(Q[:rows_n, cols], 2))
                top = rmax(scores)
                ex = jnp.exp2((scores - top) * (0.125 * LOG2E))
                prob = (ex * (1.0 / rsum(ex, 0))).astype(BF16)
                ATT[:rows_n, cols] = unstack_heads(mm(VT[cols, :], prob), 2).astype(BF16)

        loop(ed // 128 // pairs, heads2)

        def out_cols(j):
            cols = blk(j, 512)
            acc = src[q_rows, cols].astype(F32) + mm(ATT[:rows_n, :], w_a[3 * ed:4 * ed, cols])
            H1[:rows_n, cols] = (acc + evec[6, layer:layer + 1, cols]).astype(BF16)

        loop(ed // 512, out_cols)
        wait_down()
        norm_rows(H1, A, rows_n, vec(2), vec(3), 0, 0)

        def up_cols(j):
            acc = mm(A[:rows_n, :], w_up[:, blk(j, ed)])
            HM[:rows_n, blk(j, ed)] = gelu(acc + evec[8 + j, layer:layer + 1, :]).astype(BF16)

        loop(w_up.shape[1] // ed, up_cols)
        o_rows = pl.ds(pl.multiple_of(dst_start, rows_n), rows_n)

        def down_cols(j):
            cols = blk(j, 256)
            acc = H1[:rows_n, cols].astype(F32) + mm(HM[:rows_n, :], w_down[:, cols])
            dst[o_rows, cols] = (acc + evec[7, layer:layer + 1, cols]).astype(BF16)

        loop(ed // 256, down_cols)

    for cp in ld_a:
        cp.wait()
    ld_e = load(w2.at[1], X0, 8)

    def mid0():
        ld_e.start()
        for d in order:
            g1[1](d)
        for cp in ld_b:
            cp.wait()

    hv = nvis // CORES
    enc_layer(0, X0, Y0, Z0, E, H2, hv, core * hv, core * hv, 8,
              rows0, mid0)
    h_mine = pl.ds(pl.multiple_of(core * hv, hv), hv)
    swap = rcopy(H2.at[h_mine], H2.at[h_mine], s_e.at[60], r_e.at[60], t, partner)
    swap.start()
    dh = w_dec.shape[0]
    ld_f = []
    for l in range(2):
        ld_f.append(load(dqkv.at[l], Z0.at[l * d_w:(l + 1) * d_w, :dd], 9 + l))
        ld_f.append(load(dwo.at[l], Z0.at[2 * d_w + l * dd:2 * d_w + (l + 1) * dd, :dd], 11 + l))
        ld_f.append(load(dw1.at[l], Y0.at[l * dd:(l + 1) * dd, :4 * dd], 13 + l))
        ld_f.append(load(dw2.at[l], Z0.at[l * 4 * dd:(l + 1) * 4 * dd, dd:2 * dd], 15 + l))
    ld_dec = load(w_dec, Y0.at[:dh, 6 * dd:7 * dd], 18)
    ld_dec.start()
    for cp in ld_f:
        cp.start()
    for cp in ld_c:
        cp.wait()

    def mid1():
        for d in order:
            for e in order:
                g1[2](d, e)
        ld_d.wait()
        ld_e.wait()

    def rows1(vec):
        norm_rows(H2, A, hv, vec(0), vec(1), core * hv, core * hv)
        other = pl.ds(pl.multiple_of((1 - core) * hv, hv), hv)
        rcopy(H2.at[other], H2.at[other], s_e.at[60], r_e.at[60], t, partner).wait_recv()
        norm_rows(H2, A, hv, vec(0), vec(1), (1 - core) * hv, (1 - core) * hv)

    enc_layer(1, X1, Y1, X0, H2, E2, vis_blk, t * vis_blk, 0, 8, rows1, mid1)
    norm_rows(E2, A, vis_blk, efin[:1, :], efin[1:2, :], 0, 0)
    ld_dec.wait()
    z_mine = Z.at[t, :vis_blk]
    Z[t, :vis_blk] = mm(A[:vis_blk, :], Y0[:dh, 6 * dd:7 * dd]).astype(BF16)
    stz = []
    for d in range(1, nt):
        stz.append(rcopy(z_mine, z_mine, s_e.at[56 + d], r_e.at[56 + d], tpeer(d), r))
    for cp in stz:
        cp.start()
    for tb in range(nt):
        IC[tb] = index_cols(MB[tb])
    for d in range(nt):
        for e in range(nx):
            g1[3](d, e)
    for cp in ld_f:
        cp.wait()

    groups = dd // 128
    heads_g = 4
    stack = heads_g * tok
    scale = float(dd // (groups * heads_g)) ** -0.5 * LOG2E
    blk_tok = nr * tok

    pick = iota((tok, 128), 1)

    def one_hot(column):
        return jnp.where(column == pick.astype(F32), 1.0, 0.0).astype(BF16)

    own_col = rsum(jnp.where(pick == r, IC[t, :tok, :], 0.0), 1)
    hidden = (mm(one_hot(own_col), Z[t]) + DP[t, r].astype(F32)).astype(BF16)

    def start_attention(layer, normed):
        base = layer * d_w
        q_all = (mm_t(normed, Z0[base:base + dd, :dd]) + dvec[4, layer:layer + 1, :]).astype(BF16)
        for g in range(groups):
            QB[g] = head_rows(q_all[:, g * 128:(g + 1) * 128], heads_g)
        OT[...] = jnp.zeros(OT.shape, F32)
        ML[:groups] = jnp.full((groups, 1, stack), -jnp.inf, F32)
        ML[groups:2 * groups] = jnp.zeros((groups, 1, stack), F32)

    def attend(layer, rows):
        base = layer * d_w
        keys = mm_t(rows, Z0[base + dd:base + 2 * dd, :dd]).astype(BF16)
        acc = mm_t(Z0[base + 2 * dd:base + 3 * dd, :dd], rows)
        bias = column_of(dvec[5, layer:layer + 1, :], 128)
        values = (acc + jnp.concatenate([bias] * (rows.shape[0] // 128), axis=1)).astype(BF16)
        for g in range(groups):
            sc = mm_t(keys[:, g * 128:(g + 1) * 128], QB[g])
            old = ML[g]
            top = jnp.maximum(old, rmax(sc))
            ex = jnp.exp2((sc - top) * scale)
            keep = jnp.exp2((old - top) * scale)
            ML[g] = top
            ML[groups + g] = ML[groups + g] * keep + rsum(ex, 0)
            lanes = slice(g * 128, (g + 1) * 128)
            OT[lanes, :] = OT[lanes, :] * keep + mm(values[lanes, :], ex.astype(BF16))

    def finish_block(layer, hidden):
        for g in range(groups):
            lanes = slice(g * 128, (g + 1) * 128)
            ATT[:tok, lanes] = unstack_heads(OT[lanes, :] * (1.0 / ML[groups + g]), heads_g).astype(BF16)
        wo_rows = 2 * d_w + layer * dd
        acc = hidden.astype(F32) + mm(ATT[:tok, :dd], Z0[wo_rows:wo_rows + dd, :dd]) + dvec[6, layer:layer + 1, :]
        resid = acc.astype(BF16)
        normed = norm(resid, dvec[2, layer:layer + 1, :], dvec[3, layer:layer + 1, :])
        for j in range(4):
            cols = slice(j * dd, (j + 1) * dd)
            up = mm(normed, Y0[layer * dd:(layer + 1) * dd, cols])
            HM[:tok, cols] = gelu(up + dvec[8 + j, layer:layer + 1, :]).astype(BF16)
        down = mm(HM[:tok, :4 * dd], Z0[layer * 4 * dd:(layer + 1) * 4 * dd, dd:2 * dd])
        return (resid.astype(F32) + down + dvec[7, layer:layer + 1, :]).astype(BF16)

    start_attention(0, norm(hidden, dvec[0, :1, :], dvec[1, :1, :]))

    def first_rows(d):
        tb = tsrc(d)
        if d > 0:
            ref = Z.at[tb, :vis_blk]
            rcopy(ref, ref, s_e.at[56 + d], r_e.at[56 + d], t, partner).wait_recv()
        cols_t = IC[tb]
        for q in range(nr):
            u = (mm(one_hot(cols_t[:tok, q:q + 1]), Z[tb]) + DP[tb, q].astype(F32)).astype(BF16)
            HD[d, q * tok:(q + 1) * tok, :] = norm(u, dvec[0, :1, :], dvec[1, :1, :])

    first_rows(0)
    for d in range(1, nt):
        first_rows(d)
        attend(0, HD[d - 1])
    attend(0, HD[nt - 1])
    hidden = finish_block(0, hidden)
    A2[t, r] = norm(hidden, dvec[0, 1:2, :], dvec[1, 1:2, :])
    H1[:tok, :dd] = hidden
    g2 = gather(A2, s_h, r_h)
    g2[0]()
    start_attention(1, A2[t, r])

    def unit(*chips):
        parts = []
        for d, e in chips:
            g2[3](d, e)
            xs = lax.rem(x + nx - e, nx) * CORES
            parts.append(A2[tsrc(d), pl.ds(xs, CORES)].reshape(CORES * tok, dd))
        attend(1, jnp.concatenate(parts, axis=0))

    for d in order:
        g2[1](d)
    unit((0, 0), (1, 0), (3, 0), (0, 1))
    unit((0, 3), (2, 0), (0, 2))
    near = [(1, 1), (1, 3), (3, 1), (3, 3)]
    far = [(1, 2), (2, 1), (2, 3), (3, 2), (2, 2)]
    for d, e in near + far:
        g2[2](d, e)
    unit(*near)
    unit(*far)
    hidden = finish_block(1, H1[:tok, :dd])
    out[...] = norm(hidden, dfin[:1, :], dfin[1:2, :])

    for cp in st + st2 + fw2 + stz + [swap]:
        cp.wait_send()
    g1[4]()
    g2[4]()


def solution(mesh):
    nt, nr = mesh.shape["time"], mesh.shape["region"]

    def local_step(patches, enc_pos, vis_mask, dec_pos, w_embed, b_embed, enc_vec, enc_wqkv, enc_wo, enc_w1, enc_w2, enc_final, w_dec_in, mask_token, dec_vec, dec_wqkv, dec_wo, dec_w1, dec_w2, dec_final, w_out):
        tok = patches.shape[0]
        ed, dd = w_embed.shape[1], w_dec_in.shape[1]
        layers = enc_vec.shape[0]
        nvis = tok * nt * nr // KEEP_DIV
        flat = lambda w, width: jnp.transpose(w, (0, 2, 3, 4, 1)).reshape(layers, 3 * width, width)
        small = [patches, enc_pos, vis_mask.reshape(1, tok), b_embed.reshape(1, ed), dec_pos,
                 jnp.transpose(enc_vec, (1, 0, 2)), enc_final, mask_token.reshape(dd // 128, 128),
                 jnp.transpose(dec_vec, (1, 0, 2)), dec_final]
        big = [w_embed, flat(enc_wqkv, ed), enc_wo.reshape(layers, ed, ed), enc_w1, enc_w2, w_dec_in,
               flat(dec_wqkv, dd), dec_wo.reshape(layers, dd, dd), dec_w1, dec_w2]
        scratch = [pltpu.VMEM(v.shape, v.dtype) for v in small] + [
            pltpu.VMEM((4 * ed, ed), BF16), pltpu.VMEM((4 * ed, ed), BF16),
            pltpu.VMEM((ed, 4 * ed), BF16), pltpu.VMEM((ed, 4 * ed), BF16), pltpu.VMEM((4 * ed, ed), BF16),
            pltpu.VMEM((CORES, tok // 2, ed // CORES), BF16), pltpu.VMEM((nr, tok // 2, ed // CORES), BF16), pltpu.VMEM((nr, 8, 128), F32), pltpu.VMEM((nt, nr, 128), F32),
            pltpu.VMEM((nvis, ed), BF16), pltpu.VMEM((nvis // nt, ed), BF16), pltpu.VMEM((nvis // CORES, ed), BF16), pltpu.VMEM((nvis, ed), BF16),
            pltpu.VMEM((nvis, ed), BF16), pltpu.VMEM((nvis // CORES, ed), BF16), pltpu.VMEM((nvis, ed), BF16),
            pltpu.VMEM((ed, nvis), BF16), pltpu.VMEM((nvis // CORES, ed), BF16), pltpu.VMEM((nvis // CORES, 4 * ed), BF16),
            pltpu.VMEM((nt, 128, dd), BF16), pltpu.VMEM((nt, 128, 128), F32),
            pltpu.VMEM((nt, nr, tok, dd), BF16), pltpu.VMEM((nt, nr, tok, dd), BF16),
            pltpu.VMEM((nt, nr * tok, dd), BF16), pltpu.VMEM((dd // 128, 4 * tok, 128), BF16),
            pltpu.VMEM((dd, 4 * tok), F32), pltpu.VMEM((2 * dd // 128, 1, 4 * tok), F32),
        ] + [pltpu.SemaphoreType.DMA((n,)) for n in (16, 24) + (64,) * 6]
        rows = pl.pallas_call(
            functools.partial(kernel, nt, nr, len(small)),
            out_shape=jax.ShapeDtypeStruct((tok, dd), BF16),
            in_specs=[pl.BlockSpec(memory_space=pl.ANY)] * (len(small) + len(big)),
            out_specs=pl.BlockSpec(memory_space=pltpu.VMEM),
            scratch_shapes=scratch,
            compiler_params=pltpu.CompilerParams(collective_id=0, has_side_effects=True, vmem_limit_bytes=64 * 1024 * 1024 - 65536),
            name="mae",
        )(*small, *big)
        return mm(rows, w_out)

    token_rows = P(TOKEN_AXES, None)
    token_flags = P(TOKEN_AXES)
    replicated = P()
    in_specs = (token_rows, token_rows, token_flags, token_rows) + (replicated,) * 17
    return jax.shard_map(local_step, mesh=mesh, in_specs=in_specs, out_specs=token_rows, check_vma=False)
```

```python
import functools
import jax
import jax.numpy as jnp
from jax import lax
from jax.experimental import pallas as pl
from jax.experimental.pallas import tpu as pltpu
from jax.sharding import PartitionSpec as P

KEEP_DIV = 8
LN_EPS = 1e-6
CORES = 2
TOKEN_AXES = ("batch", "time", "region")
MESH_ID = pl.DeviceIdType.MESH
F32 = jnp.float32
BF16 = jnp.bfloat16
LOG2E = 1.4426950408889634


def mm(lhs, rhs):
    return jnp.dot(lhs, rhs, preferred_element_type=F32)


def mm_t(lhs, rhs):
    return lax.dot_general(lhs, rhs, (((1,), (1,)), ((), ())), preferred_element_type=F32)


def norm(rows, gain, shift):
    rows = rows.astype(F32)
    centered = rows - jnp.mean(rows, axis=-1, keepdims=True)
    variance = jnp.mean(centered * centered, axis=-1, keepdims=True)
    return (centered * lax.rsqrt(variance + LN_EPS) * gain + shift).astype(BF16)


def gelu(val):
    return 0.5 * val * (1.0 + lax.erf(val * 0.7071067811865476))


def loop(count, body):
    lax.fori_loop(0, count, lambda i, c: (body(i), c)[1], 0)


def blk(i, size):
    return pl.ds(pl.multiple_of(i * size, size), size)


def column_of(row, lanes):
    return jnp.broadcast_to(row, (lanes, row.shape[1])).T


def head_rows(q_rows, heads):
    lanes = q_rows.shape[1]
    head = iota(q_rows.shape, 1) // (lanes // heads)
    return jnp.concatenate([jnp.where(head == h, q_rows, jnp.zeros_like(q_rows)) for h in range(heads)], axis=0)


def unstack_heads(out_t, heads):
    out = out_t.T
    rows = out.shape[0] // heads
    head = iota((rows, out.shape[1]), 1) // (out.shape[1] // heads)
    total = jnp.where(head == 0, out[:rows], 0.0)
    for h in range(1, heads):
        total = total + jnp.where(head == h, out[h * rows:(h + 1) * rows], 0.0)
    return total


def rsum(val, axis):
    return jnp.sum(val, axis=axis, keepdims=True)


def rmax(val):
    return jnp.max(val, axis=0, keepdims=True)


def iota(shape, axis):
    return lax.broadcasted_iota(jnp.int32, shape, axis)


def kernel(nt, nr, count, *refs):
    given, refs = refs[:count], refs[count:]
    w_embed, wqkv, wo, w1, w2, w_dec, dqkv, dwo, dw1, dw2, out = refs[:11]
    held, refs = refs[11:11 + count], refs[11 + count:]
    (X0, X1, Y0, Y1, Z0, SS, SL, MT, MB, E, E2, H1, H2, A, Q, K, VT, ATT, HM, Z, IC, DP, A2, HD, QB, OT, ML,
     isem, wsem, s_e, r_e, s_g, r_g, s_h, r_h) = refs
    patches, enc_pos, vis, b_embed, dec_pos, evec, efin, mtok, dvec, dfin = held
    ld_in = [pltpu.make_async_copy(src, dst, isem.at[i]) for i, (src, dst) in enumerate(zip(given, held))]
    for cp in ld_in[2:3] + ld_in[:2]:
        cp.start()
    t = lax.axis_index("time")
    r = lax.axis_index("region")
    nx = nr // CORES
    x, core = r // CORES, lax.rem(r, CORES)
    partner = r + 1 - 2 * core
    tok = patches.shape[0]
    slots = SL.shape[2]
    vis_blk = E.shape[0] // nt
    ed, dd = E.shape[1], dec_pos.shape[1]
    nvis = E.shape[0]

    def xpeer(dx):
        return lax.rem(x + dx, nx) * CORES + core

    def tpeer(dy):
        return lax.rem(t + dy, nt)

    def xsrc(dx):
        return lax.rem(x + nx - dx, nx) * CORES + core

    def tsrc(dy):
        return lax.rem(t + nt - dy, nt)

    def rcopy(src, dst, ssem, rsem, tt, rr):
        return pltpu.make_async_remote_copy(src_ref=src, dst_ref=dst, send_sem=ssem, recv_sem=rsem,
                                            device_id={"time": tt, "region": rr}, device_id_type=MESH_ID)

    def load(src, dst, i):
        return pltpu.make_async_copy(src, dst, wsem.at[i])

    quarter = ed // 4
    subs = range(2)
    chunks = [half * 2 + sub for sub in subs for half in range(CORES)]
    ld_embed = {}
    for j in chunks:
        cols = slice(j * quarter, (j + 1) * quarter)
        ld_embed[j] = load(w_embed.at[:, cols], Y1.at[:w_embed.shape[0], cols], 20 + j)
        ld_embed[j].start()
    for cp in ld_in[3:]:
        cp.start()

    barrier = pltpu.get_barrier_semaphore()
    order = [d for d in (1, 3, 2) if d < nx]
    across = [(t, partner, 1 - core)] + [(t, xpeer(d) + f * (1 - 2 * core), core + f * (1 - 2 * core)) for d in order for f in range(CORES)]
    peers = [p[:2] for p in across] + [(tpeer(d), r) for d in range(1, nt)]
    for tt, rr in peers:
        pl.semaphore_signal(barrier, inc=1, device_id={"time": tt, "region": rr}, device_id_type=MESH_ID)

    ld_in[2].wait()
    mask_row = vis[...].astype(F32)
    mask_pad = jnp.concatenate([mask_row, jnp.zeros((1, 128 - tok), F32)], axis=1)
    mask_pad = jnp.broadcast_to(mask_pad, (8, 128))
    MT[r] = mask_pad
    tri = (iota((128, 128), 0) < iota((128, 128), 1)).astype(BF16)
    local_rank = mm(mask_pad.astype(BF16), tri)[:1, :tok]
    selector = jnp.where((local_rank == iota((slots, tok), 0).astype(F32)) & (mask_row == 1.0), 1.0, 0.0).astype(BF16)
    for cp in ld_in[:2] + ld_in[3:]:
        cp.wait()

    qkv_w, d_w = 3 * ed, 3 * dd
    ld_a = [load(wqkv.at[0], X0.at[:qkv_w], 1), load(wo.at[0], X0.at[qkv_w:qkv_w + ed], 2)]
    ld_b = [load(w1.at[0], Y0, 3), load(w2.at[0], Z0, 4)]
    ld_c = [load(wqkv.at[1], X1.at[:qkv_w], 5), load(wo.at[1], X1.at[qkv_w:qkv_w + ed], 6)]
    def embed_chunk(j):
        ld_embed[j].wait()
        cols = slice(j * quarter, (j + 1) * quarter)
        emb = (mm(patches[...], Y1[:patches.shape[1], cols]) + b_embed[:, cols] + enc_pos[:, cols].astype(F32)).astype(BF16)
        SS[j] = mm(selector, emb).astype(BF16)

    st = []
    for sub in subs:
        for half in range(CORES):
            embed_chunk(half * 2 + sub)
        SL[sub, r] = SS[core * 2 + sub]
        if sub == 0:
            pl.semaphore_wait(barrier, len(peers))
        for i, (tt, rr, half) in enumerate(across):
            st.append(rcopy(SS.at[half * 2 + sub], SL.at[sub, r], s_e.at[16 * sub + i], r_e.at[16 * sub + i], tt, rr))
            st[-1].start()
            if sub == 0:
                st.append(rcopy(MT.at[r], MT.at[r], s_e.at[8 + i], r_e.at[8 + i], tt, rr))
                st[-1].start()
    ld_d = load(w1.at[1], Y1, 7)
    for cp in ld_a + ld_b + ld_c + [ld_d]:
        cp.start()
    token_row = jnp.broadcast_to(jnp.concatenate([mtok[i:i + 1, :] for i in range(dd // 128)], axis=1), (128 - vis_blk, dd))
    for tb in range(nt):
        Z[tb, vis_blk:128] = token_row
    DP[t, r] = dec_pos[...]
    sources = [partner] + [xsrc(d) + f * (1 - 2 * core) for d in order for f in range(CORES)]

    def slots_arrive(sub):
        for i, src in enumerate(sources):
            got = SL.at[sub, src]
            rcopy(got, got, s_e.at[16 * sub + i], r_e.at[16 * sub + i], t, partner).wait_recv()

    slots_arrive(0)
    for i, src in enumerate(sources):
        rcopy(MT.at[src], MT.at[src], s_e.at[8 + i], r_e.at[8 + i], t, partner).wait_recv()

    mask_all = jnp.concatenate([MT[d, :1, :] for d in range(nr)], axis=0)
    MB[t] = mask_all
    counts = rsum(mask_all, 1)
    lane_dev = iota((nr, nr * slots), 1) // slots
    sub_dev = iota((nr, nr * slots), 0)
    lane_cnt = rsum(jnp.where(lane_dev == sub_dev, counts, 0.0), 0)
    lane_off = rsum(jnp.where(sub_dev < lane_dev, counts, 0.0), 0)
    lane_slot = lax.rem(iota((1, nr * slots), 1), slots).astype(F32)
    target = jnp.where(lane_slot < lane_cnt, lane_off + lane_slot, -1.0)
    rank_id = iota((vis_blk, nr * slots), 0).astype(F32)
    compact = jnp.where(target == rank_id, 1.0, 0.0).astype(BF16)
    my_rows = blk(t, vis_blk)


    def part(which, sub):
        return pl.ds(pl.multiple_of(which * 2 * quarter + sub * quarter, quarter), quarter)

    st2 = []
    for sub in subs:
        if sub > 0:
            slots_arrive(sub)
        E[my_rows, part(core, sub)] = mm(compact, SL[sub].reshape(nr * slots, quarter)).astype(BF16)
        mine = E.at[my_rows, part(core, sub)]
        for d in order:
            st2.append(rcopy(mine, mine, s_e.at[32 + 4 * sub + d], r_e.at[32 + 4 * sub + d], tpeer(d), r))
            if sub == 0:
                st2.append(rcopy(MB.at[t], MB.at[t], s_e.at[40 + d], r_e.at[40 + d], tpeer(d), r))
        st2.append(rcopy(mine, mine, s_e.at[48 + 4 * sub], r_e.at[48 + 4 * sub], t, partner))
        for cp in st2[-(2 * nt - 1 if sub == 0 else nt):]:
            cp.start()

    def gather(buf, ss, rs):
        hw = dd // 2
        first, second, third = [], [], {}

        def step1():
            own = buf.at[t, r]
            for d in order:
                first.append(rcopy(own, own, ss.at[d], rs.at[d], tpeer(d), r))
                first.append(rcopy(own, own, ss.at[4 + d], rs.at[4 + d], t, xpeer(d)))
            first.append(rcopy(own, own, ss.at[0], rs.at[0], t, partner))
            for cp in first:
                cp.start()

        def to_partner(ref, d, e):
            i = 40 + d * 4 + e
            cp = rcopy(ref, ref, ss.at[i], rs.at[i], t, partner)
            cp.start()
            third[(d, e)] = cp

        def step2(d):
            src = tsrc(d)
            rcopy(buf.at[src, r], buf.at[src, r], ss.at[d], rs.at[d], t, partner).wait_recv()
            for e in range(1, nx):
                i = 8 + d * 4 + e
                low = buf.at[src, r, :, :hw]
                second.append(rcopy(low, low, ss.at[i], rs.at[i], t, xpeer(e)))
                second[-1].start()
            to_partner(buf.at[src, r], d, 0)
            src = xsrc(d)
            rcopy(buf.at[t, src], buf.at[t, src], ss.at[4 + d], rs.at[4 + d], t, partner).wait_recv()
            for e in range(1, nt):
                i = 24 + d * 4 + e
                high = buf.at[t, src, :, hw:]
                second.append(rcopy(high, high, ss.at[i], rs.at[i], tpeer(e), r))
                second[-1].start()
            to_partner(buf.at[t, src], 0, d)

        def step3(d, e):
            ref = buf.at[tsrc(d), xsrc(e)]
            low, high = ref.at[:, :hw], ref.at[:, hw:]
            rcopy(low, low, ss.at[8 + d * 4 + e], rs.at[8 + d * 4 + e], t, partner).wait_recv()
            rcopy(high, high, ss.at[24 + e * 4 + d], rs.at[24 + e * 4 + d], t, partner).wait_recv()
            to_partner(ref, d, e)

        def finish(d, e):
            if d == 0 and e == 0:
                rcopy(buf.at[t, partner], buf.at[t, partner], ss.at[0], rs.at[0], t, partner).wait_recv()
            else:
                third[(d, e)].wait_recv()

        def drain():
            for cp in first + second + list(third.values()):
                cp.wait_send()

        return step1, step2, step3, finish, drain

    g1 = gather(DP, s_g, r_g)

    def index_cols(masks):
        ranks = mm(masks.astype(BF16), tri)
        sub, lane = iota((nr, nr), 0), iota((nr, nr), 1)
        cnt_lane = rsum(jnp.where(sub == lane, rsum(masks, 1), 0.0), 0)
        off = rsum(jnp.where(lane < sub, cnt_lane, 0.0), 1)
        index = jnp.where(masks == 1.0, ranks + off, float(vis_blk))
        return jnp.concatenate([index, jnp.zeros((128 - nr, 128), F32)], axis=0).T

    def norm_rows(src, dst, count, gain, shift, start, dst_start, step=64):
        def body(i):
            rows = pl.ds(pl.multiple_of(start + i * step, step), step)
            dst[pl.ds(pl.multiple_of(dst_start + i * step, step), step), :] = norm(src[rows, :], gain, shift)
        loop(count // step, body)

    fw2 = []

    def rows0(vec):
        def take(block, i):
            for sub in subs:
                got = E.at[blk(block, vis_blk), part(1 - core, sub)]
                rcopy(got, got, s_e.at[48 + 4 * sub + i], r_e.at[48 + 4 * sub + i], t, partner).wait_recv()
            norm_rows(E, A, vis_blk, vec(0), vec(1), block * vis_blk, block * vis_blk)

        take(t, 0)
        for sub in subs:
            for d in order:
                got = E.at[blk(tsrc(d), vis_blk), part(core, sub)]
                rcopy(got, got, s_e.at[32 + 4 * sub + d], r_e.at[32 + 4 * sub + d], t, partner).wait_recv()
                fw2.append(rcopy(got, got, s_e.at[48 + 4 * sub + d], r_e.at[48 + 4 * sub + d], t, partner))
                fw2[-1].start()
        g1[0]()
        for d in order:
            rcopy(MB.at[tsrc(d)], MB.at[tsrc(d)], s_e.at[40 + d], r_e.at[40 + d], t, partner).wait_recv()
            take(tsrc(d), d)

    def project(dst, rows_n, src_rows, w, w_row, bias):
        def body(j):
            cols = blk(j, 512)
            acc = mm_t(A[src_rows, :], w[pl.ds(pl.multiple_of(w_row + j * 512, 512), 512), :])
            if bias is not None:
                acc = acc + bias(cols)
            dst[:rows_n, cols] = acc.astype(BF16)
        loop(ed // 512, body)

    def enc_layer(layer, w_a, w_up, w_down, src, dst, rows_n, start, dst_start, pairs, wait_rows, wait_down):
        def vec(i):
            return evec[i, layer:layer + 1, :]

        wait_rows(vec)
        q_rows = pl.ds(pl.multiple_of(start, rows_n), rows_n)
        project(Q, rows_n, q_rows, w_a, 0, lambda cols: evec[4, layer:layer + 1, cols])
        project(K, nvis, slice(None), w_a, ed, None)

        def v_rows(j):
            rows = blk(j, 512)
            bias = column_of(evec[5, layer:layer + 1, rows], 128)
            acc = mm_t(w_a[pl.ds(pl.multiple_of(2 * ed + j * 512, 512), 512), :], A[...])
            VT[rows, :] = (acc + jnp.concatenate([bias] * (nvis // 128), axis=1)).astype(BF16)

        loop(ed // 512, v_rows)

        def heads2(p):
            for q in range(pairs):
                cols = blk(p * pairs + q, 128)
                scores = mm_t(K[:, cols], head_rows(Q[:rows_n, cols], 2))
                top = rmax(scores)
                ex = jnp.exp2((scores - top) * (0.125 * LOG2E))
                prob = (ex * (1.0 / rsum(ex, 0))).astype(BF16)
                ATT[:rows_n, cols] = unstack_heads(mm(VT[cols, :], prob), 2).astype(BF16)

        loop(ed // 128 // pairs, heads2)

        def out_cols(j):
            cols = blk(j, 512)
            acc = src[q_rows, cols].astype(F32) + mm(ATT[:rows_n, :], w_a[3 * ed:4 * ed, cols])
            H1[:rows_n, cols] = (acc + evec[6, layer:layer + 1, cols]).astype(BF16)

        loop(ed // 512, out_cols)
        wait_down()
        norm_rows(H1, A, rows_n, vec(2), vec(3), 0, 0)

        def up_cols(j):
            acc = mm(A[:rows_n, :], w_up[:, blk(j, ed)])
            HM[:rows_n, blk(j, ed)] = gelu(acc + evec[8 + j, layer:layer + 1, :]).astype(BF16)

        loop(w_up.shape[1] // ed, up_cols)
        o_rows = pl.ds(pl.multiple_of(dst_start, rows_n), rows_n)

        def down_cols(j):
            cols = blk(j, 256)
            acc = H1[:rows_n, cols].astype(F32) + mm(HM[:rows_n, :], w_down[:, cols])
            dst[o_rows, cols] = (acc + evec[7, layer:layer + 1, cols]).astype(BF16)

        loop(ed // 256, down_cols)

    for cp in ld_a:
        cp.wait()
    ld_e = load(w2.at[1], X0, 8)

    def mid0():
        ld_e.start()
        for d in order:
            g1[1](d)
        for cp in ld_b:
            cp.wait()

    hv = nvis // CORES
    enc_layer(0, X0, Y0, Z0, E, H2, hv, core * hv, core * hv, 8,
              rows0, mid0)
    h_mine = pl.ds(pl.multiple_of(core * hv, hv), hv)
    swap = rcopy(H2.at[h_mine], H2.at[h_mine], s_e.at[60], r_e.at[60], t, partner)
    swap.start()
    dh = w_dec.shape[0]
    ld_f = []
    for l in range(2):
        ld_f.append(load(dqkv.at[l], Z0.at[l * d_w:(l + 1) * d_w, :dd], 9 + l))
        ld_f.append(load(dwo.at[l], Z0.at[2 * d_w + l * dd:2 * d_w + (l + 1) * dd, :dd], 11 + l))
        ld_f.append(load(dw1.at[l], Y0.at[l * dd:(l + 1) * dd, :4 * dd], 13 + l))
        ld_f.append(load(dw2.at[l], Z0.at[l * 4 * dd:(l + 1) * 4 * dd, dd:2 * dd], 15 + l))
    ld_dec = load(w_dec, Y0.at[:dh, 6 * dd:7 * dd], 18)
    ld_dec.start()
    for cp in ld_f:
        cp.start()
    for cp in ld_c:
        cp.wait()

    def mid1():
        for d in order:
            for e in order:
                g1[2](d, e)
        ld_d.wait()
        ld_e.wait()

    def rows1(vec):
        norm_rows(H2, A, hv, vec(0), vec(1), core * hv, core * hv)
        other = pl.ds(pl.multiple_of((1 - core) * hv, hv), hv)
        rcopy(H2.at[other], H2.at[other], s_e.at[60], r_e.at[60], t, partner).wait_recv()
        norm_rows(H2, A, hv, vec(0), vec(1), (1 - core) * hv, (1 - core) * hv)

    enc_layer(1, X1, Y1, X0, H2, E2, vis_blk, t * vis_blk, 0, 8, rows1, mid1)
    norm_rows(E2, A, vis_blk, efin[:1, :], efin[1:2, :], 0, 0)
    ld_dec.wait()
    z_mine = Z.at[t, :vis_blk]
    Z[t, :vis_blk] = mm(A[:vis_blk, :], Y0[:dh, 6 * dd:7 * dd]).astype(BF16)
    stz = []
    for d in range(1, nt):
        stz.append(rcopy(z_mine, z_mine, s_e.at[56 + d], r_e.at[56 + d], tpeer(d), r))
    for cp in stz:
        cp.start()
    for tb in range(nt):
        IC[tb] = index_cols(MB[tb])
    for d in range(nt):
        for e in range(nx):
            g1[3](d, e)
    for cp in ld_f:
        cp.wait()

    groups = dd // 128
    heads_g = 4
    stack = heads_g * tok
    scale = float(dd // (groups * heads_g)) ** -0.5 * LOG2E
    blk_tok = nr * tok

    pick = iota((tok, 128), 1)

    def one_hot(column):
        return jnp.where(column == pick.astype(F32), 1.0, 0.0).astype(BF16)

    own_col = rsum(jnp.where(pick == r, IC[t, :tok, :], 0.0), 1)
    hidden = (mm(one_hot(own_col), Z[t]) + DP[t, r].astype(F32)).astype(BF16)

    def start_attention(layer, normed):
        base = layer * d_w
        q_all = (mm_t(normed, Z0[base:base + dd, :dd]) + dvec[4, layer:layer + 1, :]).astype(BF16)
        for g in range(groups):
            QB[g] = head_rows(q_all[:, g * 128:(g + 1) * 128], heads_g)
        OT[...] = jnp.zeros(OT.shape, F32)
        ML[:groups] = jnp.full((groups, 1, stack), -jnp.inf, F32)
        ML[groups:2 * groups] = jnp.zeros((groups, 1, stack), F32)

    def attend(layer, rows):
        base = layer * d_w
        keys = mm_t(rows, Z0[base + dd:base + 2 * dd, :dd]).astype(BF16)
        acc = mm_t(Z0[base + 2 * dd:base + 3 * dd, :dd], rows)
        bias = column_of(dvec[5, layer:layer + 1, :], 128)
        values = (acc + jnp.concatenate([bias] * (rows.shape[0] // 128), axis=1)).astype(BF16)
        for g in range(groups):
            sc = mm_t(keys[:, g * 128:(g + 1) * 128], QB[g])
            old = ML[g]
            top = jnp.maximum(old, rmax(sc))
            ex = jnp.exp2((sc - top) * scale)
            keep = jnp.exp2((old - top) * scale)
            ML[g] = top
            ML[groups + g] = ML[groups + g] * keep + rsum(ex, 0)
            lanes = slice(g * 128, (g + 1) * 128)
            OT[lanes, :] = OT[lanes, :] * keep + mm(values[lanes, :], ex.astype(BF16))

    def finish_block(layer, hidden):
        for g in range(groups):
            lanes = slice(g * 128, (g + 1) * 128)
            ATT[:tok, lanes] = unstack_heads(OT[lanes, :] * (1.0 / ML[groups + g]), heads_g).astype(BF16)
        wo_rows = 2 * d_w + layer * dd
        acc = hidden.astype(F32) + mm(ATT[:tok, :dd], Z0[wo_rows:wo_rows + dd, :dd]) + dvec[6, layer:layer + 1, :]
        resid = acc.astype(BF16)
        normed = norm(resid, dvec[2, layer:layer + 1, :], dvec[3, layer:layer + 1, :])
        for j in range(4):
            cols = slice(j * dd, (j + 1) * dd)
            up = mm(normed, Y0[layer * dd:(layer + 1) * dd, cols])
            HM[:tok, cols] = gelu(up + dvec[8 + j, layer:layer + 1, :]).astype(BF16)
        down = mm(HM[:tok, :4 * dd], Z0[layer * 4 * dd:(layer + 1) * 4 * dd, dd:2 * dd])
        return (resid.astype(F32) + down + dvec[7, layer:layer + 1, :]).astype(BF16)

    start_attention(0, norm(hidden, dvec[0, :1, :], dvec[1, :1, :]))

    def first_unit(d):
        tb = tsrc(d)
        ref = Z.at[tb, :vis_blk]

        @pl.when(d > 0)
        def _():
            rcopy(ref, ref, s_e.at[56 + d], r_e.at[56 + d], t, partner).wait_recv()

        cols_t = IC[tb]
        for q in range(nr):
            u = (mm(one_hot(cols_t[:tok, q:q + 1]), Z[tb]) + DP[tb, q].astype(F32)).astype(BF16)
            HD[q * tok:(q + 1) * tok, :] = norm(u, dvec[0, :1, :], dvec[1, :1, :])
        attend(0, HD[...])

    loop(nt, first_unit)
    hidden = finish_block(0, hidden)
    A2[t, r] = norm(hidden, dvec[0, 1:2, :], dvec[1, 1:2, :])
    H1[:tok, :dd] = hidden
    g2 = gather(A2, s_h, r_h)
    g2[0]()
    start_attention(1, A2[t, r])

    def unit(*chips):
        parts = []
        for d, e in chips:
            g2[3](d, e)
            xs = lax.rem(x + nx - e, nx) * CORES
            parts.append(A2[tsrc(d), pl.ds(xs, CORES)].reshape(CORES * tok, dd))
        attend(1, jnp.concatenate(parts, axis=0))

    for d in order:
        g2[1](d)
    near = [(d, e) for d in order[:2] for e in order[:2]]
    far = [(d, e) for d in order for e in order if (d, e) not in near]
    unit((0, 0), (1, 0), (3, 0), (0, 1))
    for d, e in near:
        g2[2](d, e)
    unit((0, 3), (2, 0), (0, 2))
    for d, e in far:
        g2[2](d, e)
    unit(*near)
    unit(*far)
    hidden = finish_block(1, H1[:tok, :dd])
    out[...] = norm(hidden, dfin[:1, :], dfin[1:2, :])

    for cp in st + st2 + fw2 + stz + [swap]:
        cp.wait_send()
    g1[4]()
    g2[4]()


def solution(mesh):
    nt, nr = mesh.shape["time"], mesh.shape["region"]

    def local_step(patches, enc_pos, vis_mask, dec_pos, w_embed, b_embed, enc_vec, enc_wqkv, enc_wo, enc_w1, enc_w2, enc_final, w_dec_in, mask_token, dec_vec, dec_wqkv, dec_wo, dec_w1, dec_w2, dec_final, w_out):
        tok = patches.shape[0]
        ed, dd = w_embed.shape[1], w_dec_in.shape[1]
        layers = enc_vec.shape[0]
        nvis = tok * nt * nr // KEEP_DIV
        flat = lambda w, width: jnp.transpose(w, (0, 2, 3, 4, 1)).reshape(layers, 3 * width, width)
        small = [patches, enc_pos, vis_mask.reshape(1, tok), b_embed.reshape(1, ed), dec_pos,
                 jnp.transpose(enc_vec, (1, 0, 2)), enc_final, mask_token.reshape(dd // 128, 128),
                 jnp.transpose(dec_vec, (1, 0, 2)), dec_final]
        big = [w_embed, flat(enc_wqkv, ed), enc_wo.reshape(layers, ed, ed), enc_w1, enc_w2, w_dec_in,
               flat(dec_wqkv, dd), dec_wo.reshape(layers, dd, dd), dec_w1, dec_w2]
        scratch = [pltpu.VMEM(v.shape, v.dtype) for v in small] + [
            pltpu.VMEM((4 * ed, ed), BF16), pltpu.VMEM((4 * ed, ed), BF16),
            pltpu.VMEM((ed, 4 * ed), BF16), pltpu.VMEM((ed, 4 * ed), BF16), pltpu.VMEM((4 * ed, ed), BF16),
            pltpu.VMEM((4, tok // 2, ed // 4), BF16), pltpu.VMEM((2, nr, tok // 2, ed // 4), BF16), pltpu.VMEM((nr, 8, 128), F32), pltpu.VMEM((nt, nr, 128), F32),
            pltpu.VMEM((nvis, ed), BF16), pltpu.VMEM((nvis // nt, ed), BF16), pltpu.VMEM((nvis // CORES, ed), BF16), pltpu.VMEM((nvis, ed), BF16),
            pltpu.VMEM((nvis, ed), BF16), pltpu.VMEM((nvis // CORES, ed), BF16), pltpu.VMEM((nvis, ed), BF16),
            pltpu.VMEM((ed, nvis), BF16), pltpu.VMEM((nvis // CORES, ed), BF16), pltpu.VMEM((nvis // CORES, 4 * ed), BF16),
            pltpu.VMEM((nt, 128, dd), BF16), pltpu.VMEM((nt, 128, 128), F32),
            pltpu.VMEM((nt, nr, tok, dd), BF16), pltpu.VMEM((nt, nr, tok, dd), BF16),
            pltpu.VMEM((nr * tok, dd), BF16), pltpu.VMEM((dd // 128, 4 * tok, 128), BF16),
            pltpu.VMEM((dd, 4 * tok), F32), pltpu.VMEM((2 * dd // 128, 1, 4 * tok), F32),
        ] + [pltpu.SemaphoreType.DMA((n,)) for n in (16, 24) + (64,) * 6]
        rows = pl.pallas_call(
            functools.partial(kernel, nt, nr, len(small)),
            out_shape=jax.ShapeDtypeStruct((tok, dd), BF16),
            in_specs=[pl.BlockSpec(memory_space=pl.ANY)] * (len(small) + len(big)),
            out_specs=pl.BlockSpec(memory_space=pltpu.VMEM),
            scratch_shapes=scratch,
            compiler_params=pltpu.CompilerParams(collective_id=0, has_side_effects=True, vmem_limit_bytes=64 * 1024 * 1024 - 65536),
            name="mae",
        )(*small, *big)
        return mm(rows, w_out)

    token_rows = P(TOKEN_AXES, None)
    token_flags = P(TOKEN_AXES)
    replicated = P()
    in_specs = (token_rows, token_rows, token_flags, token_rows) + (replicated,) * 17
    return jax.shard_map(local_step, mesh=mesh, in_specs=in_specs, out_specs=token_rows, check_vma=False)
```

```python
import functools
import jax
import jax.numpy as jnp
from jax import lax
from jax.experimental import pallas as pl
from jax.experimental.pallas import tpu as pltpu
from jax.sharding import PartitionSpec as P

KEEP_DIV = 8
LN_EPS = 1e-6
CORES = 2
TOKEN_AXES = ("batch", "time", "region")
MESH_ID = pl.DeviceIdType.MESH
F32 = jnp.float32
BF16 = jnp.bfloat16
LOG2E = 1.4426950408889634


def mm(lhs, rhs):
    return jnp.dot(lhs, rhs, preferred_element_type=F32)


def mm_t(lhs, rhs):
    return lax.dot_general(lhs, rhs, (((1,), (1,)), ((), ())), preferred_element_type=F32)


def norm(rows, gain, shift):
    rows = rows.astype(F32)
    centered = rows - jnp.mean(rows, axis=-1, keepdims=True)
    variance = jnp.mean(centered * centered, axis=-1, keepdims=True)
    return (centered * lax.rsqrt(variance + LN_EPS) * gain + shift).astype(BF16)


def gelu(val):
    return 0.5 * val * (1.0 + lax.erf(val * 0.7071067811865476))


def loop(count, body):
    lax.fori_loop(0, count, lambda i, c: (body(i), c)[1], 0)


def blk(i, size):
    return pl.ds(pl.multiple_of(i * size, size), size)


def column_of(row, lanes):
    return jnp.broadcast_to(row, (lanes, row.shape[1])).T


def head_rows(q_rows, heads):
    lanes = q_rows.shape[1]
    head = iota(q_rows.shape, 1) // (lanes // heads)
    return jnp.concatenate([jnp.where(head == h, q_rows, jnp.zeros_like(q_rows)) for h in range(heads)], axis=0)


def unstack_heads(out_t, heads):
    out = out_t.T
    rows = out.shape[0] // heads
    head = iota((rows, out.shape[1]), 1) // (out.shape[1] // heads)
    total = jnp.where(head == 0, out[:rows], 0.0)
    for h in range(1, heads):
        total = total + jnp.where(head == h, out[h * rows:(h + 1) * rows], 0.0)
    return total


def rsum(val, axis):
    return jnp.sum(val, axis=axis, keepdims=True)


def rmax(val):
    return jnp.max(val, axis=0, keepdims=True)


def iota(shape, axis):
    return lax.broadcasted_iota(jnp.int32, shape, axis)


def kernel(nt, nr, count, *refs):
    given, refs = refs[:count], refs[count:]
    w_embed, wqkv, wo, w1, w2, w_dec, dqkv, dwo, dw1, dw2, out = refs[:11]
    held, refs = refs[11:11 + count], refs[11 + count:]
    (X0, X1, Y0, Y1, Z0, SS, SL, MT, MB, E, E2, H1, H2, A, Q, K, VT, ATT, HM, Z, IC, DP, A2, HD, QB, OT, ML,
     isem, wsem, s_e, r_e, s_g, r_g, s_h, r_h) = refs
    patches, enc_pos, vis, b_embed, dec_pos, evec, efin, mtok, dvec, dfin = held
    ld_in = [pltpu.make_async_copy(src, dst, isem.at[i]) for i, (src, dst) in enumerate(zip(given, held))]
    for cp in ld_in[2:3] + ld_in[:2]:
        cp.start()
    t = lax.axis_index("time")
    r = lax.axis_index("region")
    nx = nr // CORES
    x, core = r // CORES, lax.rem(r, CORES)
    partner = r + 1 - 2 * core
    tok = patches.shape[0]
    slots = SL.shape[2]
    vis_blk = E.shape[0] // nt
    ed, dd = E.shape[1], dec_pos.shape[1]
    nvis = E.shape[0]

    def xpeer(dx):
        return lax.rem(x + dx, nx) * CORES + core

    def tpeer(dy):
        return lax.rem(t + dy, nt)

    def xsrc(dx):
        return lax.rem(x + nx - dx, nx) * CORES + core

    def tsrc(dy):
        return lax.rem(t + nt - dy, nt)

    def rcopy(src, dst, ssem, rsem, tt, rr):
        return pltpu.make_async_remote_copy(src_ref=src, dst_ref=dst, send_sem=ssem, recv_sem=rsem,
                                            device_id={"time": tt, "region": rr}, device_id_type=MESH_ID)

    def load(src, dst, i):
        return pltpu.make_async_copy(src, dst, wsem.at[i])

    quarter = ed // 4
    subs = range(2)
    chunks = [half * 2 + sub for sub in subs for half in range(CORES)]
    ld_embed = {}
    for j in chunks:
        cols = slice(j * quarter, (j + 1) * quarter)
        ld_embed[j] = load(w_embed.at[:, cols], Y1.at[:w_embed.shape[0], cols], 20 + j)
        ld_embed[j].start()
    for cp in ld_in[3:]:
        cp.start()

    barrier = pltpu.get_barrier_semaphore()
    order = [d for d in (1, 3, 2) if d < nx]
    across = [(t, partner, 1 - core)] + [(t, xpeer(d) + f * (1 - 2 * core), core + f * (1 - 2 * core)) for d in order for f in range(CORES)]
    peers = [p[:2] for p in across] + [(tpeer(d), r) for d in range(1, nt)]
    for tt, rr in peers:
        pl.semaphore_signal(barrier, inc=1, device_id={"time": tt, "region": rr}, device_id_type=MESH_ID)

    ld_in[2].wait()
    mask_row = vis[...].astype(F32)
    mask_pad = jnp.concatenate([mask_row, jnp.zeros((1, 128 - tok), F32)], axis=1)
    mask_pad = jnp.broadcast_to(mask_pad, (8, 128))
    MT[r] = mask_pad
    tri = (iota((128, 128), 0) < iota((128, 128), 1)).astype(BF16)
    local_rank = mm(mask_pad.astype(BF16), tri)[:1, :tok]
    selector = jnp.where((local_rank == iota((slots, tok), 0).astype(F32)) & (mask_row == 1.0), 1.0, 0.0).astype(BF16)
    for cp in ld_in[:2] + ld_in[3:]:
        cp.wait()

    qkv_w, d_w = 3 * ed, 3 * dd
    ld_a = [load(wqkv.at[0], X0.at[:qkv_w], 1), load(wo.at[0], X0.at[qkv_w:qkv_w + ed], 2)]
    ld_b = [load(w1.at[0], Y0, 3), load(w2.at[0], Z0, 4)]
    ld_c = [load(wqkv.at[1], X1.at[:qkv_w], 5), load(wo.at[1], X1.at[qkv_w:qkv_w + ed], 6)]
    def embed_chunk(j):
        ld_embed[j].wait()
        cols = slice(j * quarter, (j + 1) * quarter)
        emb = (mm(patches[...], Y1[:patches.shape[1], cols]) + b_embed[:, cols] + enc_pos[:, cols].astype(F32)).astype(BF16)
        SS[j] = mm(selector, emb).astype(BF16)

    st = []
    for sub in subs:
        for half in range(CORES):
            embed_chunk(half * 2 + sub)
        SL[sub, r] = SS[core * 2 + sub]
        if sub == 0:
            pl.semaphore_wait(barrier, len(peers))
        for i, (tt, rr, half) in enumerate(across):
            st.append(rcopy(SS.at[half * 2 + sub], SL.at[sub, r], s_e.at[16 * sub + i], r_e.at[16 * sub + i], tt, rr))
            st[-1].start()
            if sub == 0:
                st.append(rcopy(MT.at[r], MT.at[r], s_e.at[8 + i], r_e.at[8 + i], tt, rr))
                st[-1].start()
    ld_d = load(w1.at[1], Y1, 7)
    for cp in ld_a + ld_b + ld_c + [ld_d]:
        cp.start()
    token_row = jnp.broadcast_to(jnp.concatenate([mtok[i:i + 1, :] for i in range(dd // 128)], axis=1), (128 - vis_blk, dd))
    for tb in range(nt):
        Z[tb, vis_blk:128] = token_row
    DP[t, r] = dec_pos[...]
    sources = [partner] + [xsrc(d) + f * (1 - 2 * core) for d in order for f in range(CORES)]

    def slots_arrive(sub):
        for i, src in enumerate(sources):
            got = SL.at[sub, src]
            rcopy(got, got, s_e.at[16 * sub + i], r_e.at[16 * sub + i], t, partner).wait_recv()

    slots_arrive(0)
    for i, src in enumerate(sources):
        rcopy(MT.at[src], MT.at[src], s_e.at[8 + i], r_e.at[8 + i], t, partner).wait_recv()

    mask_all = jnp.concatenate([MT[d, :1, :] for d in range(nr)], axis=0)
    MB[t] = mask_all
    counts = rsum(mask_all, 1)
    lane_dev = iota((nr, nr * slots), 1) // slots
    sub_dev = iota((nr, nr * slots), 0)
    lane_cnt = rsum(jnp.where(lane_dev == sub_dev, counts, 0.0), 0)
    lane_off = rsum(jnp.where(sub_dev < lane_dev, counts, 0.0), 0)
    lane_slot = lax.rem(iota((1, nr * slots), 1), slots).astype(F32)
    target = jnp.where(lane_slot < lane_cnt, lane_off + lane_slot, -1.0)
    rank_id = iota((vis_blk, nr * slots), 0).astype(F32)
    compact = jnp.where(target == rank_id, 1.0, 0.0).astype(BF16)
    my_rows = blk(t, vis_blk)


    def part(which, sub):
        return pl.ds(pl.multiple_of(which * 2 * quarter + sub * quarter, quarter), quarter)

    st2 = []
    for sub in subs:
        if sub > 0:
            slots_arrive(sub)
        E[my_rows, part(core, sub)] = mm(compact, SL[sub].reshape(nr * slots, quarter)).astype(BF16)
        mine = E.at[my_rows, part(core, sub)]
        for d in order:
            st2.append(rcopy(mine, mine, s_e.at[32 + 4 * sub + d], r_e.at[32 + 4 * sub + d], tpeer(d), r))
            if sub == 0:
                st2.append(rcopy(MB.at[t], MB.at[t], s_e.at[40 + d], r_e.at[40 + d], tpeer(d), r))
        st2.append(rcopy(mine, mine, s_e.at[48 + 4 * sub], r_e.at[48 + 4 * sub], t, partner))
        for cp in st2[-(2 * nt - 1 if sub == 0 else nt):]:
            cp.start()

    def gather(buf, ss, rs):
        hw = dd // 2
        first, second, third = [], [], {}

        def step1():
            own = buf.at[t, r]
            for d in order:
                first.append(rcopy(own, own, ss.at[d], rs.at[d], tpeer(d), r))
                first.append(rcopy(own, own, ss.at[4 + d], rs.at[4 + d], t, xpeer(d)))
            first.append(rcopy(own, own, ss.at[0], rs.at[0], t, partner))
            for cp in first:
                cp.start()

        def to_partner(ref, d, e):
            i = 40 + d * 4 + e
            cp = rcopy(ref, ref, ss.at[i], rs.at[i], t, partner)
            cp.start()
            third[(d, e)] = cp

        def step2(d):
            src = tsrc(d)
            rcopy(buf.at[src, r], buf.at[src, r], ss.at[d], rs.at[d], t, partner).wait_recv()
            for e in range(1, nx):
                i = 8 + d * 4 + e
                low = buf.at[src, r, :, :hw]
                second.append(rcopy(low, low, ss.at[i], rs.at[i], t, xpeer(e)))
                second[-1].start()
            to_partner(buf.at[src, r], d, 0)
            src = xsrc(d)
            rcopy(buf.at[t, src], buf.at[t, src], ss.at[4 + d], rs.at[4 + d], t, partner).wait_recv()
            for e in range(1, nt):
                i = 24 + d * 4 + e
                high = buf.at[t, src, :, hw:]
                second.append(rcopy(high, high, ss.at[i], rs.at[i], tpeer(e), r))
                second[-1].start()
            to_partner(buf.at[t, src], 0, d)

        def step3(d, e):
            ref = buf.at[tsrc(d), xsrc(e)]
            low, high = ref.at[:, :hw], ref.at[:, hw:]
            rcopy(low, low, ss.at[8 + d * 4 + e], rs.at[8 + d * 4 + e], t, partner).wait_recv()
            rcopy(high, high, ss.at[24 + e * 4 + d], rs.at[24 + e * 4 + d], t, partner).wait_recv()
            to_partner(ref, d, e)

        def finish(d, e):
            if d == 0 and e == 0:
                rcopy(buf.at[t, partner], buf.at[t, partner], ss.at[0], rs.at[0], t, partner).wait_recv()
            else:
                third[(d, e)].wait_recv()

        def drain():
            for cp in first + second + list(third.values()):
                cp.wait_send()

        return step1, step2, step3, finish, drain

    g1 = gather(DP, s_g, r_g)

    def index_cols(masks):
        ranks = mm(masks.astype(BF16), tri)
        sub, lane = iota((nr, nr), 0), iota((nr, nr), 1)
        cnt_lane = rsum(jnp.where(sub == lane, rsum(masks, 1), 0.0), 0)
        off = rsum(jnp.where(lane < sub, cnt_lane, 0.0), 1)
        index = jnp.where(masks == 1.0, ranks + off, float(vis_blk))
        return jnp.concatenate([index, jnp.zeros((128 - nr, 128), F32)], axis=0).T

    def norm_rows(src, dst, count, gain, shift, start, dst_start, step=64):
        def body(i):
            rows = pl.ds(pl.multiple_of(start + i * step, step), step)
            dst[pl.ds(pl.multiple_of(dst_start + i * step, step), step), :] = norm(src[rows, :], gain, shift)
        loop(count // step, body)

    fw2 = []

    def rows0(vec):
        def take(block, i):
            for sub in subs:
                got = E.at[blk(block, vis_blk), part(1 - core, sub)]
                rcopy(got, got, s_e.at[48 + 4 * sub + i], r_e.at[48 + 4 * sub + i], t, partner).wait_recv()
            norm_rows(E, A, vis_blk, vec(0), vec(1), block * vis_blk, block * vis_blk)

        take(t, 0)
        for sub in subs:
            for d in order:
                got = E.at[blk(tsrc(d), vis_blk), part(core, sub)]
                rcopy(got, got, s_e.at[32 + 4 * sub + d], r_e.at[32 + 4 * sub + d], t, partner).wait_recv()
                fw2.append(rcopy(got, got, s_e.at[48 + 4 * sub + d], r_e.at[48 + 4 * sub + d], t, partner))
                fw2[-1].start()
        g1[0]()
        for d in order:
            rcopy(MB.at[tsrc(d)], MB.at[tsrc(d)], s_e.at[40 + d], r_e.at[40 + d], t, partner).wait_recv()
            take(tsrc(d), d)

    def enc_layer(layer, w_a, w_up, w_down, src, dst, rows_n, start, dst_start, pairs, wait_rows, wait_down):
        def vec(i):
            return evec[i, layer:layer + 1, :]

        wait_rows(vec)
        q_rows = pl.ds(pl.multiple_of(start, rows_n), rows_n)

        def qkv_cols(j):
            cols = blk(j, 512)

            def w_rows(which):
                return w_a[pl.ds(pl.multiple_of(which * ed + j * 512, 512), 512), :]

            Q[:rows_n, cols] = (mm_t(A[q_rows, :], w_rows(0)) + evec[4, layer:layer + 1, cols]).astype(BF16)
            K[:, cols] = mm_t(A[...], w_rows(1)).astype(BF16)
            bias = column_of(evec[5, layer:layer + 1, cols], 128)
            VT[cols, :] = (mm_t(w_rows(2), A[...]) + jnp.concatenate([bias] * (nvis // 128), axis=1)).astype(BF16)

        loop(ed // 512, qkv_cols)

        def heads2(p):
            for q in range(pairs):
                cols = blk(p * pairs + q, 128)
                scores = mm_t(K[:, cols], head_rows(Q[:rows_n, cols], 2))
                top = rmax(scores)
                ex = jnp.exp2((scores - top) * (0.125 * LOG2E))
                prob = (ex * (1.0 / rsum(ex, 0))).astype(BF16)
                ATT[:rows_n, cols] = unstack_heads(mm(VT[cols, :], prob), 2).astype(BF16)

        loop(ed // 128 // pairs, heads2)

        def out_cols(j):
            cols = blk(j, 512)
            acc = src[q_rows, cols].astype(F32) + mm(ATT[:rows_n, :], w_a[3 * ed:4 * ed, cols])
            H1[:rows_n, cols] = (acc + evec[6, layer:layer + 1, cols]).astype(BF16)

        loop(ed // 512, out_cols)
        wait_down()
        norm_rows(H1, A, rows_n, vec(2), vec(3), 0, 0)

        def up_cols(j):
            acc = mm(A[:rows_n, :], w_up[:, blk(j, ed)])
            HM[:rows_n, blk(j, ed)] = gelu(acc + evec[8 + j, layer:layer + 1, :]).astype(BF16)

        loop(w_up.shape[1] // ed, up_cols)
        o_rows = pl.ds(pl.multiple_of(dst_start, rows_n), rows_n)

        def down_cols(j):
            cols = blk(j, 512)
            acc = H1[:rows_n, cols].astype(F32) + mm(HM[:rows_n, :], w_down[:, cols])
            dst[o_rows, cols] = (acc + evec[7, layer:layer + 1, cols]).astype(BF16)

        loop(ed // 512, down_cols)

    for cp in ld_a:
        cp.wait()
    ld_e = load(w2.at[1], X0, 8)

    def mid0():
        ld_e.start()
        for d in order:
            g1[1](d)
        for cp in ld_b:
            cp.wait()

    hv = nvis // CORES
    enc_layer(0, X0, Y0, Z0, E, H2, hv, core * hv, core * hv, 8,
              rows0, mid0)
    h_mine = pl.ds(pl.multiple_of(core * hv, hv), hv)
    swap = rcopy(H2.at[h_mine], H2.at[h_mine], s_e.at[60], r_e.at[60], t, partner)
    swap.start()
    dh = w_dec.shape[0]
    ld_f = []
    for l in range(2):
        ld_f.append(load(dqkv.at[l], Z0.at[l * d_w:(l + 1) * d_w, :dd], 9 + l))
        ld_f.append(load(dwo.at[l], Z0.at[2 * d_w + l * dd:2 * d_w + (l + 1) * dd, :dd], 11 + l))
        ld_f.append(load(dw1.at[l], Y0.at[l * dd:(l + 1) * dd, :4 * dd], 13 + l))
        ld_f.append(load(dw2.at[l], Z0.at[l * 4 * dd:(l + 1) * 4 * dd, dd:2 * dd], 15 + l))
    ld_dec = load(w_dec, Y0.at[:dh, 6 * dd:7 * dd], 18)
    ld_dec.start()
    for cp in ld_f:
        cp.start()
    for cp in ld_c:
        cp.wait()

    def mid1():
        for d in order:
            for e in order:
                g1[2](d, e)
        ld_d.wait()
        ld_e.wait()

    def rows1(vec):
        norm_rows(H2, A, hv, vec(0), vec(1), core * hv, core * hv)
        other = pl.ds(pl.multiple_of((1 - core) * hv, hv), hv)
        rcopy(H2.at[other], H2.at[other], s_e.at[60], r_e.at[60], t, partner).wait_recv()
        norm_rows(H2, A, hv, vec(0), vec(1), (1 - core) * hv, (1 - core) * hv)

    enc_layer(1, X1, Y1, X0, H2, E2, vis_blk, t * vis_blk, 0, 8, rows1, mid1)
    norm_rows(E2, A, vis_blk, efin[:1, :], efin[1:2, :], 0, 0)
    ld_dec.wait()
    z_mine = Z.at[t, :vis_blk]
    Z[t, :vis_blk] = mm(A[:vis_blk, :], Y0[:dh, 6 * dd:7 * dd]).astype(BF16)
    stz = []
    for d in range(1, nt):
        stz.append(rcopy(z_mine, z_mine, s_e.at[56 + d], r_e.at[56 + d], tpeer(d), r))
    for cp in stz:
        cp.start()
    for tb in range(nt):
        IC[tb] = index_cols(MB[tb])
    for d in range(nt):
        for e in range(nx):
            g1[3](d, e)
    for cp in ld_f:
        cp.wait()

    groups = dd // 128
    heads_g = 4
    stack = heads_g * tok
    scale = float(dd // (groups * heads_g)) ** -0.5 * LOG2E
    blk_tok = nr * tok

    pick = iota((tok, 128), 1)

    def one_hot(column):
        return jnp.where(column == pick.astype(F32), 1.0, 0.0).astype(BF16)

    own_col = rsum(jnp.where(pick == r, IC[t, :tok, :], 0.0), 1)
    hidden = (mm(one_hot(own_col), Z[t]) + DP[t, r].astype(F32)).astype(BF16)

    def start_attention(layer, normed):
        base = layer * d_w
        q_all = (mm_t(normed, Z0[base:base + dd, :dd]) + dvec[4, layer:layer + 1, :]).astype(BF16)
        for g in range(groups):
            QB[g] = head_rows(q_all[:, g * 128:(g + 1) * 128], heads_g)
        OT[...] = jnp.zeros(OT.shape, F32)
        ML[:groups] = jnp.full((groups, 1, stack), -jnp.inf, F32)
        ML[groups:2 * groups] = jnp.zeros((groups, 1, stack), F32)

    def attend(layer, rows):
        base = layer * d_w
        keys = mm_t(rows, Z0[base + dd:base + 2 * dd, :dd]).astype(BF16)
        acc = mm_t(Z0[base + 2 * dd:base + 3 * dd, :dd], rows)
        bias = column_of(dvec[5, layer:layer + 1, :], 128)
        values = (acc + jnp.concatenate([bias] * (rows.shape[0] // 128), axis=1)).astype(BF16)
        for g in range(groups):
            sc = mm_t(keys[:, g * 128:(g + 1) * 128], QB[g])
            old = ML[g]
            top = jnp.maximum(old, rmax(sc))
            ex = jnp.exp2((sc - top) * scale)
            keep = jnp.exp2((old - top) * scale)
            ML[g] = top
            ML[groups + g] = ML[groups + g] * keep + rsum(ex, 0)
            lanes = slice(g * 128, (g + 1) * 128)
            OT[lanes, :] = OT[lanes, :] * keep + mm(values[lanes, :], ex.astype(BF16))

    def finish_block(layer, hidden):
        for g in range(groups):
            lanes = slice(g * 128, (g + 1) * 128)
            ATT[:tok, lanes] = unstack_heads(OT[lanes, :] * (1.0 / ML[groups + g]), heads_g).astype(BF16)
        wo_rows = 2 * d_w + layer * dd
        acc = hidden.astype(F32) + mm(ATT[:tok, :dd], Z0[wo_rows:wo_rows + dd, :dd]) + dvec[6, layer:layer + 1, :]
        resid = acc.astype(BF16)
        normed = norm(resid, dvec[2, layer:layer + 1, :], dvec[3, layer:layer + 1, :])
        for j in range(4):
            cols = slice(j * dd, (j + 1) * dd)
            up = mm(normed, Y0[layer * dd:(layer + 1) * dd, cols])
            HM[:tok, cols] = gelu(up + dvec[8 + j, layer:layer + 1, :]).astype(BF16)
        down = mm(HM[:tok, :4 * dd], Z0[layer * 4 * dd:(layer + 1) * 4 * dd, dd:2 * dd])
        return (resid.astype(F32) + down + dvec[7, layer:layer + 1, :]).astype(BF16)

    start_attention(0, norm(hidden, dvec[0, :1, :], dvec[1, :1, :]))

    def first_unit(d):
        tb = tsrc(d)
        ref = Z.at[tb, :vis_blk]

        @pl.when(d > 0)
        def _():
            rcopy(ref, ref, s_e.at[56 + d], r_e.at[56 + d], t, partner).wait_recv()

        cols_t = IC[tb]
        for q in range(nr):
            u = (mm(one_hot(cols_t[:tok, q:q + 1]), Z[tb]) + DP[tb, q].astype(F32)).astype(BF16)
            HD[q * tok:(q + 1) * tok, :] = norm(u, dvec[0, :1, :], dvec[1, :1, :])
        attend(0, HD[...])

    loop(nt, first_unit)
    hidden = finish_block(0, hidden)
    A2[t, r] = norm(hidden, dvec[0, 1:2, :], dvec[1, 1:2, :])
    H1[:tok, :dd] = hidden
    g2 = gather(A2, s_h, r_h)
    g2[0]()
    start_attention(1, A2[t, r])

    def unit(*chips):
        parts = []
        for d, e in chips:
            g2[3](d, e)
            xs = lax.rem(x + nx - e, nx) * CORES
            parts.append(A2[tsrc(d), pl.ds(xs, CORES)].reshape(CORES * tok, dd))
        attend(1, jnp.concatenate(parts, axis=0))

    for d in order:
        g2[1](d)
    near = [(d, e) for d in order[:2] for e in order[:2]]
    far = [(d, e) for d in order for e in order if (d, e) not in near]
    unit((0, 0), (1, 0), (3, 0), (0, 1))
    for d, e in near:
        g2[2](d, e)
    unit((0, 3), (2, 0), (0, 2))
    for d, e in far:
        g2[2](d, e)
    unit(*near)
    unit(*far)
    hidden = finish_block(1, H1[:tok, :dd])
    out[...] = norm(hidden, dfin[:1, :], dfin[1:2, :])

    for cp in st + st2 + fw2 + stz + [swap]:
        cp.wait_send()
    g1[4]()
    g2[4]()


def solution(mesh):
    nt, nr = mesh.shape["time"], mesh.shape["region"]

    def local_step(patches, enc_pos, vis_mask, dec_pos, w_embed, b_embed, enc_vec, enc_wqkv, enc_wo, enc_w1, enc_w2, enc_final, w_dec_in, mask_token, dec_vec, dec_wqkv, dec_wo, dec_w1, dec_w2, dec_final, w_out):
        tok = patches.shape[0]
        ed, dd = w_embed.shape[1], w_dec_in.shape[1]
        layers = enc_vec.shape[0]
        nvis = tok * nt * nr // KEEP_DIV
        flat = lambda w, width: jnp.transpose(w, (0, 2, 3, 4, 1)).reshape(layers, 3 * width, width)
        small = [patches, enc_pos, vis_mask.reshape(1, tok), b_embed.reshape(1, ed), dec_pos,
                 jnp.transpose(enc_vec, (1, 0, 2)), enc_final, mask_token.reshape(dd // 128, 128),
                 jnp.transpose(dec_vec, (1, 0, 2)), dec_final]
        big = [w_embed, flat(enc_wqkv, ed), enc_wo.reshape(layers, ed, ed), enc_w1, enc_w2, w_dec_in,
               flat(dec_wqkv, dd), dec_wo.reshape(layers, dd, dd), dec_w1, dec_w2]
        scratch = [pltpu.VMEM(v.shape, v.dtype) for v in small] + [
            pltpu.VMEM((4 * ed, ed), BF16), pltpu.VMEM((4 * ed, ed), BF16),
            pltpu.VMEM((ed, 4 * ed), BF16), pltpu.VMEM((ed, 4 * ed), BF16), pltpu.VMEM((4 * ed, ed), BF16),
            pltpu.VMEM((4, tok // 2, ed // 4), BF16), pltpu.VMEM((2, nr, tok // 2, ed // 4), BF16), pltpu.VMEM((nr, 8, 128), F32), pltpu.VMEM((nt, nr, 128), F32),
            pltpu.VMEM((nvis, ed), BF16), pltpu.VMEM((nvis // nt, ed), BF16), pltpu.VMEM((nvis // CORES, ed), BF16), pltpu.VMEM((nvis, ed), BF16),
            pltpu.VMEM((nvis, ed), BF16), pltpu.VMEM((nvis // CORES, ed), BF16), pltpu.VMEM((nvis, ed), BF16),
            pltpu.VMEM((ed, nvis), BF16), pltpu.VMEM((nvis // CORES, ed), BF16), pltpu.VMEM((nvis // CORES, 4 * ed), BF16),
            pltpu.VMEM((nt, 128, dd), BF16), pltpu.VMEM((nt, 128, 128), F32),
            pltpu.VMEM((nt, nr, tok, dd), BF16), pltpu.VMEM((nt, nr, tok, dd), BF16),
            pltpu.VMEM((nr * tok, dd), BF16), pltpu.VMEM((dd // 128, 4 * tok, 128), BF16),
            pltpu.VMEM((dd, 4 * tok), F32), pltpu.VMEM((2 * dd // 128, 1, 4 * tok), F32),
        ] + [pltpu.SemaphoreType.DMA((n,)) for n in (16, 24) + (64,) * 6]
        rows = pl.pallas_call(
            functools.partial(kernel, nt, nr, len(small)),
            out_shape=jax.ShapeDtypeStruct((tok, dd), BF16),
            in_specs=[pl.BlockSpec(memory_space=pl.ANY)] * (len(small) + len(big)),
            out_specs=pl.BlockSpec(memory_space=pltpu.VMEM),
            scratch_shapes=scratch,
            compiler_params=pltpu.CompilerParams(collective_id=0, has_side_effects=True, vmem_limit_bytes=58 * 1024 * 1024),
            name="mae",
        )(*small, *big)
        return mm(rows, w_out)

    token_rows = P(TOKEN_AXES, None)
    token_flags = P(TOKEN_AXES)
    replicated = P()
    in_specs = (token_rows, token_rows, token_flags, token_rows) + (replicated,) * 17
    return jax.shard_map(local_step, mesh=mesh, in_specs=in_specs, out_specs=token_rows, check_vma=False)
```

```python
import functools
import jax
import jax.numpy as jnp
from jax import lax
from jax.experimental import pallas as pl
from jax.experimental.pallas import tpu as pltpu
from jax.sharding import PartitionSpec as P

KEEP_DIV = 8
LN_EPS = 1e-6
CORES = 2
TOKEN_AXES = ("batch", "time", "region")
MESH_ID = pl.DeviceIdType.MESH
F32 = jnp.float32
BF16 = jnp.bfloat16
LOG2E = 1.4426950408889634


def mm(lhs, rhs):
    return jnp.dot(lhs, rhs, preferred_element_type=F32)


def mm_t(lhs, rhs):
    return lax.dot_general(lhs, rhs, (((1,), (1,)), ((), ())), preferred_element_type=F32)


def norm(rows, gain, shift):
    rows = rows.astype(F32)
    centered = rows - jnp.mean(rows, axis=-1, keepdims=True)
    variance = jnp.mean(centered * centered, axis=-1, keepdims=True)
    return (centered * lax.rsqrt(variance + LN_EPS) * gain + shift).astype(BF16)


def gelu(val):
    return 0.5 * val * (1.0 + lax.erf(val * 0.7071067811865476))


def loop(count, body):
    lax.fori_loop(0, count, lambda i, c: (body(i), c)[1], 0)


def blk(i, size):
    return pl.ds(pl.multiple_of(i * size, size), size)


def column_of(row, lanes):
    return jnp.broadcast_to(row, (lanes, row.shape[1])).T


def head_rows(q_rows, heads):
    lanes = q_rows.shape[1]
    head = iota(q_rows.shape, 1) // (lanes // heads)
    return jnp.concatenate([jnp.where(head == h, q_rows, jnp.zeros_like(q_rows)) for h in range(heads)], axis=0)


def unstack_heads(out_t, heads):
    lanes, width = out_t.shape
    tiles, rows = width // lanes, width // heads
    own = lanes // tiles
    out = jnp.concatenate([out_t[i * own:(i + 1) * own, i * lanes:(i + 1) * lanes] for i in range(tiles)], axis=0).T
    if rows == lanes:
        return out
    odd = lax.rem(iota((rows, lanes), 1) // (lanes // heads), 2)
    return jnp.where(odd == 0, out[:rows], out[rows:])


def rsum(val, axis):
    return jnp.sum(val, axis=axis, keepdims=True)


def rmax(val):
    return jnp.max(val, axis=0, keepdims=True)


def iota(shape, axis):
    return lax.broadcasted_iota(jnp.int32, shape, axis)


def kernel(nt, nr, count, *refs):
    given, refs = refs[:count], refs[count:]
    w_embed, wqkv, wo, w1, w2, w_dec, dqkv, dwo, dw1, dw2, out = refs[:11]
    held, refs = refs[11:11 + count], refs[11 + count:]
    (X0, X1, Y0, Y1, Z0, SS, SL, MT, MB, E, E2, H1, H2, A, Q, K, VT, ATT, HM, Z, IC, DP, A2, HD, QB, OT, ML,
     isem, wsem, s_e, r_e, s_g, r_g, s_h, r_h) = refs
    patches, enc_pos, vis, b_embed, dec_pos, evec, efin, mtok, dvec, dfin = held
    ld_in = [pltpu.make_async_copy(src, dst, isem.at[i]) for i, (src, dst) in enumerate(zip(given, held))]
    early = [ld_in[i] for i in (2, 0, 1, 3)]
    for cp in early:
        cp.start()
    t = lax.axis_index("time")
    r = lax.axis_index("region")
    nx = nr // CORES
    x, core = r // CORES, lax.rem(r, CORES)
    partner = r + 1 - 2 * core
    tok = patches.shape[0]
    slots = SL.shape[2]
    vis_blk = E.shape[0] // nt
    ed, dd = E.shape[1], dec_pos.shape[1]
    nvis = E.shape[0]

    def xpeer(dx):
        return lax.rem(x + dx, nx) * CORES + core

    def tpeer(dy):
        return lax.rem(t + dy, nt)

    def xsrc(dx):
        return lax.rem(x + nx - dx, nx) * CORES + core

    def tsrc(dy):
        return lax.rem(t + nt - dy, nt)

    def rcopy(src, dst, ssem, rsem, tt, rr):
        return pltpu.make_async_remote_copy(src_ref=src, dst_ref=dst, send_sem=ssem, recv_sem=rsem,
                                            device_id={"time": tt, "region": rr}, device_id_type=MESH_ID)

    def load(src, dst, i):
        return pltpu.make_async_copy(src, dst, wsem.at[i])

    quarter = ed // 4
    subs = range(2)
    chunks = [half * 2 + sub for sub in subs for half in range(CORES)]
    ld_embed = {}
    for j in chunks:
        cols = slice(j * quarter, (j + 1) * quarter)
        ld_embed[j] = load(w_embed.at[:, cols], Y1.at[:w_embed.shape[0], cols], 20 + j)
        ld_embed[j].start()
    for cp in ld_in[4:]:
        cp.start()

    barrier = pltpu.get_barrier_semaphore()
    order = [d for d in (1, 3, 2) if d < nx]
    across = [(t, partner, 1 - core)] + [(t, xpeer(d) + f * (1 - 2 * core), core + f * (1 - 2 * core)) for d in order for f in range(CORES)]
    peers = [p[:2] for p in across] + [(tpeer(d), r) for d in range(1, nt)]
    for tt, rr in peers:
        pl.semaphore_signal(barrier, inc=1, device_id={"time": tt, "region": rr}, device_id_type=MESH_ID)

    ld_in[2].wait()
    mask_row = vis[...].astype(F32)
    mask_pad = jnp.concatenate([mask_row, jnp.zeros((1, 128 - tok), F32)], axis=1)
    mask_pad = jnp.broadcast_to(mask_pad, (8, 128))
    MT[r] = mask_pad
    tri = (iota((128, 128), 0) < iota((128, 128), 1)).astype(BF16)
    local_rank = mm(mask_pad.astype(BF16), tri)[:1, :tok]
    selector = jnp.where((local_rank == iota((slots, tok), 0).astype(F32)) & (mask_row == 1.0), 1.0, 0.0).astype(BF16)
    for cp in early[1:]:
        cp.wait()

    qkv_w, d_w = 3 * ed, 3 * dd
    ld_a = [load(wqkv.at[0], X0.at[:qkv_w], 1), load(wo.at[0], X0.at[qkv_w:qkv_w + ed], 2)]
    ld_b = [load(w1.at[0], Y0, 3), load(w2.at[0], Z0, 4)]
    ld_c = [load(wqkv.at[1], X1.at[:qkv_w], 5), load(wo.at[1], X1.at[qkv_w:qkv_w + ed], 6)]
    def embed_chunk(j):
        ld_embed[j].wait()
        cols = slice(j * quarter, (j + 1) * quarter)
        emb = (mm(patches[...], Y1[:patches.shape[1], cols]) + b_embed[:, cols] + enc_pos[:, cols].astype(F32)).astype(BF16)
        SS[j] = mm(selector, emb).astype(BF16)

    st = []
    for sub in subs:
        for half in range(CORES):
            embed_chunk(half * 2 + sub)
        SL[sub, r] = SS[core * 2 + sub]
        if sub == 0:
            pl.semaphore_wait(barrier, len(peers))
        for i, (tt, rr, half) in enumerate(across):
            st.append(rcopy(SS.at[half * 2 + sub], SL.at[sub, r], s_e.at[16 * sub + i], r_e.at[16 * sub + i], tt, rr))
            st[-1].start()
            if sub == 0:
                st.append(rcopy(MT.at[r], MT.at[r], s_e.at[8 + i], r_e.at[8 + i], tt, rr))
                st[-1].start()
    ld_d = load(w1.at[1], Y1, 7)
    for cp in ld_a + ld_b + ld_c + [ld_d]:
        cp.start()
    for cp in ld_in[4:]:
        cp.wait()
    token_row = jnp.broadcast_to(jnp.concatenate([mtok[i:i + 1, :] for i in range(dd // 128)], axis=1), (128 - vis_blk, dd))
    for tb in range(nt):
        Z[tb, vis_blk:128] = token_row
    DP[t, r] = dec_pos[...]
    sources = [partner] + [xsrc(d) + f * (1 - 2 * core) for d in order for f in range(CORES)]

    def slots_arrive(sub):
        for i, src in enumerate(sources):
            got = SL.at[sub, src]
            rcopy(got, got, s_e.at[16 * sub + i], r_e.at[16 * sub + i], t, partner).wait_recv()

    slots_arrive(0)
    for i, src in enumerate(sources):
        rcopy(MT.at[src], MT.at[src], s_e.at[8 + i], r_e.at[8 + i], t, partner).wait_recv()

    mask_all = jnp.concatenate([MT[d, :1, :] for d in range(nr)], axis=0)
    MB[t] = mask_all
    counts = rsum(mask_all, 1)
    lane_dev = iota((nr, nr * slots), 1) // slots
    sub_dev = iota((nr, nr * slots), 0)
    lane_cnt = rsum(jnp.where(lane_dev == sub_dev, counts, 0.0), 0)
    lane_off = rsum(jnp.where(sub_dev < lane_dev, counts, 0.0), 0)
    lane_slot = lax.rem(iota((1, nr * slots), 1), slots).astype(F32)
    target = jnp.where(lane_slot < lane_cnt, lane_off + lane_slot, -1.0)
    rank_id = iota((vis_blk, nr * slots), 0).astype(F32)
    compact = jnp.where(target == rank_id, 1.0, 0.0).astype(BF16)
    my_rows = blk(t, vis_blk)


    def part(which, sub):
        return pl.ds(pl.multiple_of(which * 2 * quarter + sub * quarter, quarter), quarter)

    st2 = []
    for sub in subs:
        if sub > 0:
            slots_arrive(sub)
        E[my_rows, part(core, sub)] = mm(compact, SL[sub].reshape(nr * slots, quarter)).astype(BF16)
        mine = E.at[my_rows, part(core, sub)]
        for d in order:
            st2.append(rcopy(mine, mine, s_e.at[32 + 4 * sub + d], r_e.at[32 + 4 * sub + d], tpeer(d), r))
            if sub == 0:
                st2.append(rcopy(MB.at[t], MB.at[t], s_e.at[40 + d], r_e.at[40 + d], tpeer(d), r))
        st2.append(rcopy(mine, mine, s_e.at[48 + 4 * sub], r_e.at[48 + 4 * sub], t, partner))
        for cp in st2[-(2 * nt - 1 if sub == 0 else nt):]:
            cp.start()

    def gather(buf, ss, rs):
        hw = dd // 2
        first, second, third = [], [], {}

        def step1():
            own = buf.at[t, r]
            for d in order:
                first.append(rcopy(own, own, ss.at[d], rs.at[d], tpeer(d), r))
                first.append(rcopy(own, own, ss.at[4 + d], rs.at[4 + d], t, xpeer(d)))
            first.append(rcopy(own, own, ss.at[0], rs.at[0], t, partner))
            for cp in first:
                cp.start()

        def to_partner(ref, d, e):
            i = 40 + d * 4 + e
            cp = rcopy(ref, ref, ss.at[i], rs.at[i], t, partner)
            cp.start()
            third[(d, e)] = cp

        def step2(d):
            src = tsrc(d)
            rcopy(buf.at[src, r], buf.at[src, r], ss.at[d], rs.at[d], t, partner).wait_recv()
            for e in range(1, nx):
                i = 8 + d * 4 + e
                low = buf.at[src, r, :, :hw]
                second.append(rcopy(low, low, ss.at[i], rs.at[i], t, xpeer(e)))
                second[-1].start()
            to_partner(buf.at[src, r], d, 0)
            src = xsrc(d)
            rcopy(buf.at[t, src], buf.at[t, src], ss.at[4 + d], rs.at[4 + d], t, partner).wait_recv()
            for e in range(1, nt):
                i = 24 + d * 4 + e
                high = buf.at[t, src, :, hw:]
                second.append(rcopy(high, high, ss.at[i], rs.at[i], tpeer(e), r))
                second[-1].start()
            to_partner(buf.at[t, src], 0, d)

        def step3(d, e):
            ref = buf.at[tsrc(d), xsrc(e)]
            low, high = ref.at[:, :hw], ref.at[:, hw:]
            rcopy(low, low, ss.at[8 + d * 4 + e], rs.at[8 + d * 4 + e], t, partner).wait_recv()
            rcopy(high, high, ss.at[24 + e * 4 + d], rs.at[24 + e * 4 + d], t, partner).wait_recv()
            to_partner(ref, d, e)

        def finish(d, e):
            if d == 0 and e == 0:
                rcopy(buf.at[t, partner], buf.at[t, partner], ss.at[0], rs.at[0], t, partner).wait_recv()
            else:
                third[(d, e)].wait_recv()

        def drain_links():
            for cp in first + second:
                cp.wait_send()

        def drain_partner():
            for cp in third.values():
                cp.wait_send()

        return step1, step2, step3, finish, drain_links, drain_partner

    g1 = gather(DP, s_g, r_g)

    def index_cols(masks):
        ranks = mm(masks.astype(BF16), tri)
        sub, lane = iota((nr, nr), 0), iota((nr, nr), 1)
        cnt_lane = rsum(jnp.where(sub == lane, rsum(masks, 1), 0.0), 0)
        off = rsum(jnp.where(lane < sub, cnt_lane, 0.0), 1)
        index = jnp.where(masks == 1.0, ranks + off, float(vis_blk))
        return jnp.concatenate([index, jnp.zeros((128 - nr, 128), F32)], axis=0).T

    def norm_rows(src, dst, count, gain, shift, start, dst_start, step=64):
        def body(i):
            rows = pl.ds(pl.multiple_of(start + i * step, step), step)
            dst[pl.ds(pl.multiple_of(dst_start + i * step, step), step), :] = norm(src[rows, :], gain, shift)
        loop(count // step, body)

    fw2 = []

    def rows0(vec):
        def take(block, i):
            for sub in subs:
                got = E.at[blk(block, vis_blk), part(1 - core, sub)]
                rcopy(got, got, s_e.at[48 + 4 * sub + i], r_e.at[48 + 4 * sub + i], t, partner).wait_recv()
            norm_rows(E, A, vis_blk, vec(0), vec(1), block * vis_blk, block * vis_blk)

        take(t, 0)
        IC[t] = index_cols(MB[t])
        for sub in subs:
            for d in order:
                got = E.at[blk(tsrc(d), vis_blk), part(core, sub)]
                rcopy(got, got, s_e.at[32 + 4 * sub + d], r_e.at[32 + 4 * sub + d], t, partner).wait_recv()
                fw2.append(rcopy(got, got, s_e.at[48 + 4 * sub + d], r_e.at[48 + 4 * sub + d], t, partner))
                fw2[-1].start()
        g1[0]()
        for d in order:
            rcopy(MB.at[tsrc(d)], MB.at[tsrc(d)], s_e.at[40 + d], r_e.at[40 + d], t, partner).wait_recv()
            IC[tsrc(d)] = index_cols(MB[tsrc(d)])
        for d in order:
            take(tsrc(d), d)

    def enc_layer(layer, w_a, w_up, w_down, src, dst, rows_n, start, dst_start, pairs, wait_rows, wait_down):
        def vec(i):
            return evec[i, layer:layer + 1, :]

        wait_rows(vec)
        q_rows = pl.ds(pl.multiple_of(start, rows_n), rows_n)

        def qkv_cols(j):
            cols = blk(j, 512)

            def w_rows(which):
                return w_a[pl.ds(pl.multiple_of(which * ed + j * 512, 512), 512), :]

            Q[:rows_n, cols] = (mm_t(A[q_rows, :], w_rows(0)) + evec[4, layer:layer + 1, cols]).astype(BF16)
            K[:, cols] = mm_t(A[...], w_rows(1)).astype(BF16)
            bias = column_of(evec[5, layer:layer + 1, cols], 128)
            VT[cols, :] = (mm_t(w_rows(2), A[...]) + jnp.concatenate([bias] * (nvis // 128), axis=1)).astype(BF16)

        loop(ed // 512, qkv_cols)

        def heads2(p):
            for q in range(pairs):
                cols = blk(p * pairs + q, 128)
                scores = mm_t(K[:, cols], head_rows(Q[:rows_n, cols], 2))
                top = rmax(scores)
                ex = jnp.exp2((scores - top) * (0.125 * LOG2E))
                prob = (ex * (1.0 / rsum(ex, 0))).astype(BF16)
                ATT[:rows_n, cols] = unstack_heads(mm(VT[cols, :], prob), 2).astype(BF16)

        loop(ed // 128 // pairs, heads2)

        def out_cols(j):
            cols = blk(j, 512)
            acc = src[q_rows, cols].astype(F32) + mm(ATT[:rows_n, :], w_a[3 * ed:4 * ed, cols])
            H1[:rows_n, cols] = (acc + evec[6, layer:layer + 1, cols]).astype(BF16)

        loop(ed // 512, out_cols)
        wait_down()
        norm_rows(H1, A, rows_n, vec(2), vec(3), 0, 0)

        def up_cols(j):
            acc = mm(A[:rows_n, :], w_up[:, blk(j, ed)])
            HM[:rows_n, blk(j, ed)] = gelu(acc + evec[8 + j, layer:layer + 1, :]).astype(BF16)

        loop(w_up.shape[1] // ed, up_cols)
        o_rows = pl.ds(pl.multiple_of(dst_start, rows_n), rows_n)

        def down_cols(j):
            cols = blk(j, 512)
            acc = H1[:rows_n, cols].astype(F32) + mm(HM[:rows_n, :], w_down[:, cols])
            dst[o_rows, cols] = (acc + evec[7, layer:layer + 1, cols]).astype(BF16)

        loop(ed // 512, down_cols)

    for cp in ld_a:
        cp.wait()
    ld_e = load(w2.at[1], X0, 8)

    def mid0():
        ld_e.start()
        for d in order:
            g1[1](d)
        for cp in ld_b:
            cp.wait()

    hv = nvis // CORES
    enc_layer(0, X0, Y0, Z0, E, H2, hv, core * hv, core * hv, 8,
              rows0, mid0)
    h_mine = pl.ds(pl.multiple_of(core * hv, hv), hv)
    swap = rcopy(H2.at[h_mine], H2.at[h_mine], s_e.at[60], r_e.at[60], t, partner)
    swap.start()
    dh = w_dec.shape[0]
    ld_f = []
    for l in range(2):
        ld_f.append(load(dqkv.at[l], Z0.at[l * d_w:(l + 1) * d_w, :dd], 9 + l))
        ld_f.append(load(dwo.at[l], Z0.at[2 * d_w + l * dd:2 * d_w + (l + 1) * dd, :dd], 11 + l))
        ld_f.append(load(dw1.at[l], Y0.at[l * dd:(l + 1) * dd, :4 * dd], 13 + l))
        ld_f.append(load(dw2.at[l], Z0.at[l * 4 * dd:(l + 1) * 4 * dd, dd:2 * dd], 15 + l))
    ld_dec = load(w_dec, Y0.at[:dh, 6 * dd:7 * dd], 18)
    ld_dec.start()
    for cp in ld_f:
        cp.start()
    for cp in ld_c:
        cp.wait()

    def mid1():
        for d in order:
            for e in order:
                g1[2](d, e)
        ld_d.wait()
        ld_e.wait()

    def rows1(vec):
        norm_rows(H2, A, hv, vec(0), vec(1), core * hv, core * hv)
        other = pl.ds(pl.multiple_of((1 - core) * hv, hv), hv)
        rcopy(H2.at[other], H2.at[other], s_e.at[60], r_e.at[60], t, partner).wait_recv()
        norm_rows(H2, A, hv, vec(0), vec(1), (1 - core) * hv, (1 - core) * hv)

    enc_layer(1, X1, Y1, X0, H2, E2, vis_blk, t * vis_blk, 0, 8, rows1, mid1)
    norm_rows(E2, A, vis_blk, efin[:1, :], efin[1:2, :], 0, 0)
    ld_dec.wait()
    z_mine = Z.at[t, :vis_blk]
    Z[t, :vis_blk] = mm(A[:vis_blk, :], Y0[:dh, 6 * dd:7 * dd]).astype(BF16)
    stz = []
    for d in range(1, nt):
        stz.append(rcopy(z_mine, z_mine, s_e.at[56 + d], r_e.at[56 + d], tpeer(d), r))
    for cp in stz:
        cp.start()
    for d in range(nt):
        for e in range(nx):
            g1[3](d, e)
    for cp in ld_f:
        cp.wait()

    groups = dd // 128
    heads_g = 4
    stack = heads_g * tok
    scale = float(dd // (groups * heads_g)) ** -0.5 * LOG2E
    blk_tok = nr * tok

    pick = iota((tok, 128), 1)

    def one_hot(column):
        return jnp.where(column == pick.astype(F32), 1.0, 0.0).astype(BF16)

    own_col = rsum(jnp.where(pick == r, IC[t, :tok, :], 0.0), 1)
    hidden = (mm(one_hot(own_col), Z[t]) + DP[t, r].astype(F32)).astype(BF16)

    def start_attention(layer, normed):
        base = layer * d_w
        q_all = (mm_t(normed, Z0[base:base + dd, :dd]) + dvec[4, layer:layer + 1, :]).astype(BF16)
        for g in range(groups):
            QB[g] = head_rows(q_all[:, g * 128:(g + 1) * 128], heads_g)
        OT[...] = jnp.zeros(OT.shape, F32)
        ML[:groups] = jnp.full((groups, 1, stack), -jnp.inf, F32)
        ML[groups:2 * groups] = jnp.zeros((groups, 1, stack), F32)

    def attend(layer, rows):
        base = layer * d_w
        keys = mm_t(rows, Z0[base + dd:base + 2 * dd, :dd]).astype(BF16)
        acc = mm_t(Z0[base + 2 * dd:base + 3 * dd, :dd], rows)
        bias = column_of(dvec[5, layer:layer + 1, :], 128)
        values = (acc + jnp.concatenate([bias] * (rows.shape[0] // 128), axis=1)).astype(BF16)
        for g in range(groups):
            sc = mm_t(keys[:, g * 128:(g + 1) * 128], QB[g])
            old = ML[g]
            top = jnp.maximum(old, rmax(sc))
            ex = jnp.exp2((sc - top) * scale)
            keep = jnp.exp2((old - top) * scale)
            ML[g] = top
            ML[groups + g] = ML[groups + g] * keep + rsum(ex, 0)
            lanes = slice(g * 128, (g + 1) * 128)
            OT[lanes, :] = OT[lanes, :] * keep + mm(values[lanes, :], ex.astype(BF16))

    def finish_block(layer, hidden):
        for g in range(groups):
            lanes = slice(g * 128, (g + 1) * 128)
            ATT[:tok, lanes] = unstack_heads(OT[lanes, :] * (1.0 / ML[groups + g]), heads_g).astype(BF16)
        wo_rows = 2 * d_w + layer * dd
        acc = hidden.astype(F32) + mm(ATT[:tok, :dd], Z0[wo_rows:wo_rows + dd, :dd]) + dvec[6, layer:layer + 1, :]
        resid = acc.astype(BF16)
        normed = norm(resid, dvec[2, layer:layer + 1, :], dvec[3, layer:layer + 1, :])
        for j in range(4):
            cols = slice(j * dd, (j + 1) * dd)
            up = mm(normed, Y0[layer * dd:(layer + 1) * dd, cols])
            HM[:tok, cols] = gelu(up + dvec[8 + j, layer:layer + 1, :]).astype(BF16)
        down = mm(HM[:tok, :4 * dd], Z0[layer * 4 * dd:(layer + 1) * 4 * dd, dd:2 * dd])
        return (resid.astype(F32) + down + dvec[7, layer:layer + 1, :]).astype(BF16)

    start_attention(0, norm(hidden, dvec[0, :1, :], dvec[1, :1, :]))

    def first_unit(i):
        d = i ^ (i // 2)
        tb = tsrc(d)
        ref = Z.at[tb, :vis_blk]

        @pl.when(d > 0)
        def _():
            rcopy(ref, ref, s_e.at[56 + d], r_e.at[56 + d], t, partner).wait_recv()

        cols_t = IC[tb]
        for q in range(nr):
            u = (mm(one_hot(cols_t[:tok, q:q + 1]), Z[tb]) + DP[tb, q].astype(F32)).astype(BF16)
            HD[q * tok:(q + 1) * tok, :] = norm(u, dvec[0, :1, :], dvec[1, :1, :])
        attend(0, HD[...])

    loop(nt, first_unit)
    hidden = finish_block(0, hidden)
    A2[t, r] = norm(hidden, dvec[0, 1:2, :], dvec[1, 1:2, :])
    H1[:tok, :dd] = hidden
    g2 = gather(A2, s_h, r_h)
    g2[0]()
    start_attention(1, A2[t, r])
    for cp in st + st2 + fw2 + stz + [swap]:
        cp.wait_send()
    g1[4]()
    g1[5]()

    def unit(*chips):
        parts = []
        for d, e in chips:
            g2[3](d, e)
            xs = lax.rem(x + nx - e, nx) * CORES
            parts.append(A2[tsrc(d), pl.ds(xs, CORES)].reshape(CORES * tok, dd))
        attend(1, jnp.concatenate(parts, axis=0))

    for d in order:
        g2[1](d)
    near = [(d, e) for d in order[:2] for e in order[:2]]
    far = [(d, e) for d in order for e in order if (d, e) not in near]
    unit((0, 0), (1, 0), (3, 0), (0, 1))
    for d, e in near:
        g2[2](d, e)
    unit((0, 3), (2, 0), (0, 2))
    g2[4]()
    for d, e in far:
        g2[2](d, e)
    unit(*near)
    unit(*far)
    hidden = finish_block(1, H1[:tok, :dd])
    out[...] = norm(hidden, dfin[:1, :], dfin[1:2, :])

    g2[5]()


def solution(mesh):
    nt, nr = mesh.shape["time"], mesh.shape["region"]

    def local_step(patches, enc_pos, vis_mask, dec_pos, w_embed, b_embed, enc_vec, enc_wqkv, enc_wo, enc_w1, enc_w2, enc_final, w_dec_in, mask_token, dec_vec, dec_wqkv, dec_wo, dec_w1, dec_w2, dec_final, w_out):
        tok = patches.shape[0]
        ed, dd = w_embed.shape[1], w_dec_in.shape[1]
        layers = enc_vec.shape[0]
        nvis = tok * nt * nr // KEEP_DIV
        flat = lambda w, width: jnp.transpose(w, (0, 2, 3, 4, 1)).reshape(layers, 3 * width, width)
        small = [patches, enc_pos, vis_mask.reshape(1, tok), b_embed.reshape(1, ed), dec_pos,
                 jnp.transpose(enc_vec, (1, 0, 2)), enc_final, mask_token.reshape(dd // 128, 128),
                 jnp.transpose(dec_vec, (1, 0, 2)), dec_final]
        big = [w_embed, flat(enc_wqkv, ed), enc_wo.reshape(layers, ed, ed), enc_w1, enc_w2, w_dec_in,
               flat(dec_wqkv, dd), dec_wo.reshape(layers, dd, dd), dec_w1, dec_w2]
        scratch = [pltpu.VMEM(v.shape, v.dtype) for v in small] + [
            pltpu.VMEM((4 * ed, ed), BF16), pltpu.VMEM((4 * ed, ed), BF16),
            pltpu.VMEM((ed, 4 * ed), BF16), pltpu.VMEM((ed, 4 * ed), BF16), pltpu.VMEM((4 * ed, ed), BF16),
            pltpu.VMEM((4, tok // 2, ed // 4), BF16), pltpu.VMEM((2, nr, tok // 2, ed // 4), BF16), pltpu.VMEM((nr, 8, 128), F32), pltpu.VMEM((nt, nr, 128), F32),
            pltpu.VMEM((nvis, ed), BF16), pltpu.VMEM((nvis // nt, ed), BF16), pltpu.VMEM((nvis // CORES, ed), BF16), pltpu.VMEM((nvis, ed), BF16),
            pltpu.VMEM((nvis, ed), BF16), pltpu.VMEM((nvis // CORES, ed), BF16), pltpu.VMEM((nvis, ed), BF16),
            pltpu.VMEM((ed, nvis), BF16), pltpu.VMEM((nvis // CORES, ed), BF16), pltpu.VMEM((nvis // CORES, 4 * ed), BF16),
            pltpu.VMEM((nt, 128, dd), BF16), pltpu.VMEM((nt, 128, 128), F32),
            pltpu.VMEM((nt, nr, tok, dd), BF16), pltpu.VMEM((nt, nr, tok, dd), BF16),
            pltpu.VMEM((nr * tok, dd), BF16), pltpu.VMEM((dd // 128, 4 * tok, 128), BF16),
            pltpu.VMEM((dd, 4 * tok), F32), pltpu.VMEM((2 * dd // 128, 1, 4 * tok), F32),
        ] + [pltpu.SemaphoreType.DMA((n,)) for n in (16, 24) + (64,) * 6]
        rows = pl.pallas_call(
            functools.partial(kernel, nt, nr, len(small)),
            out_shape=jax.ShapeDtypeStruct((tok, dd), BF16),
            in_specs=[pl.BlockSpec(memory_space=pl.ANY)] * (len(small) + len(big)),
            out_specs=pl.BlockSpec(memory_space=pltpu.VMEM),
            scratch_shapes=scratch,
            compiler_params=pltpu.CompilerParams(collective_id=0, has_side_effects=True, vmem_limit_bytes=58 * 1024 * 1024),
            name="mae",
        )(*small, *big)
        return mm(rows, w_out)

    token_rows = P(TOKEN_AXES, None)
    token_flags = P(TOKEN_AXES)
    replicated = P()
    in_specs = (token_rows, token_rows, token_flags, token_rows) + (replicated,) * 17
    return jax.shard_map(local_step, mesh=mesh, in_specs=in_specs, out_specs=token_rows, check_vma=False)
```
